128 devices in a mesh: section: 2 (over y_hi), dp: 64 (over z, x, y_lo, core).
Axes of the slice: x: 4, y: 4 (y_hi: 2, y_lo: 2; y = y_hi * 2 + y_lo), z: 4, core: 2. Of those that a mesh axis runs over, the one named last changes fastest.
Arguments:
- layer_inputs: bfloat16 [2, 16384, 4096], P('section', 'dp'), may hold values from -20 to 20
- norm_gain: float32 [2, 4096], P('section'), may hold values from 0.5 to 1.5
- queries: bfloat16 [2, 16384, 2048], P('section', 'dp'), may hold values from -100 to 100
- output_gradient: bfloat16 [2, 16384, 2048], P('section', 'dp'), may hold values from -6 to 6
- w_key: bfloat16 [2, 4096, 512], P('section'), may hold values from -0.09375 to 0.09375
- value_matrix: bfloat16 [2, 4096, 512], P('section'), may hold values from -0.09375 to 0.09375
- top_grad: bfloat16 [16384, 4096], P('dp'), may hold values from -6 to 6
Outputs:
- key_grad: bfloat16 [2, 4096, 512], P('section')
- value_grad: bfloat16 [2, 4096, 512], P('section')
- input_grad: bfloat16 [2, 16384, 4096], P('section', 'dp')
The draws below stay inside these ranges and needn't reach their ends.
All inputs are finite; a program needn't handle non-finite values.
Results may differ from the reference program's by a relative error of at most 0.0082.
Values may be sent and summed in bfloat16 or wider, within the bound.
No kernel may reach another device: no remote copies, remote signals or barrier semaphores. Data moves between devices by JAX's collectives and lax.ppermute only.
A program may use at most 128 MiB of HBM per device.

```python
import jax
import jax.numpy as jnp
from jax import lax

MODEL_WIDTH = 4096
HEAD_SIZE = 128
QUERY_HEADS = 16
KEY_VALUE_HEADS = 4
QUERY_PER_KEY = 4
SEQUENCE_TOKENS = 128
LAYERS_SECTION = 1
LAYER_TOTAL = 2
TOKEN_TOTAL = 16384
N_SECTION = 2
N_DP = 64


def draw_pair(key):
    key_inputs = jax.random.fold_in(key, 101)
    key_matrix = jax.random.fold_in(key, 102)
    inputs = jnp.clip(jax.random.normal(key_inputs, (LAYER_TOTAL, TOKEN_TOTAL, MODEL_WIDTH), jnp.float32), -6.0, 6.0)
    weight_arrays = jnp.clip(jax.random.normal(key_matrix, (LAYER_TOTAL, MODEL_WIDTH, KEY_VALUE_HEADS * HEAD_SIZE), jnp.float32), -6.0, 6.0) * MODEL_WIDTH ** (-0.5)
    return (inputs, weight_arrays)


def draw_layer_inputs(key, part):
    return draw_pair(key)[0].astype(jnp.bfloat16)


def draw_w_key(key, part):
    return draw_pair(key)[1].astype(jnp.bfloat16)


def draw_queries(key, part):
    base_draw = jnp.clip(jax.random.normal(jax.random.fold_in(key, 103), (LAYER_TOTAL, TOKEN_TOTAL, QUERY_HEADS * HEAD_SIZE), jnp.float32), -6.0, 6.0)
    return base_draw.astype(jnp.bfloat16)


def steps_of(own_key, dims, shards, smallest, largest):
    def one(dim, shards_of):
        draws = jax.random.uniform(jax.random.fold_in(jax.random.fold_in(own_key, 6), dim), (shards_of,), jnp.float32, smallest / len(shards), largest / len(shards))
        return jnp.repeat(jnp.exp(draws), dims[dim] // shards_of).reshape((-1,) + (1,) * (len(dims) - dim - 1))

    factor_of = one(*shards[0])
    for cut in shards[1:]:
        factor_of = factor_of * one(*cut)
    return factor_of


def scatter_about(rng, shape, spread, most, split=(), kind=jnp.bfloat16):
    entries = spread * jax.random.normal(rng, shape, jnp.float32)
    if split:
        entries = entries * steps_of(rng, shape, split, -0.22, 0.18)
    return jnp.clip(entries, -most, most).astype(kind)


def setup_inputs(seed: int = 0) -> dict:
    keys = jax.random.split(jax.random.key(seed), 8)
    layer_inputs = draw_layer_inputs(jax.random.fold_in(keys[7], 71), 0)
    norm_gain = jnp.clip(1.0 + 0.1 * jax.random.normal(keys[1], (LAYER_TOTAL, MODEL_WIDTH), jnp.float32), 0.5, 1.5)
    queries = draw_queries(jax.random.fold_in(keys[7], 71), 0)
    output_gradient = scatter_about(keys[3], (LAYER_TOTAL, TOKEN_TOTAL, QUERY_HEADS * HEAD_SIZE), 1.0, 6.0, ((0, 2), (1, 64)))
    w_key = draw_w_key(jax.random.fold_in(keys[7], 71), 0)
    value_matrix = scatter_about(keys[5], (LAYER_TOTAL, MODEL_WIDTH, KEY_VALUE_HEADS * HEAD_SIZE), MODEL_WIDTH ** -0.5, 0.09375, ((0, 2),))
    top_grad = scatter_about(keys[6], (TOKEN_TOTAL, MODEL_WIDTH), 1.0, 6.0, ((0, 64),))
    return {"layer_inputs": layer_inputs, "norm_gain": norm_gain, "queries": queries, "output_gradient": output_gradient, "w_key": w_key, "value_matrix": value_matrix, "top_grad": top_grad}


epsilon = 1e-05

def single_sequence(operands):
    query_sequence, key_sequence, value_sequence, sequence_output_gradient = operands
    scale = HEAD_SIZE ** (-0.5)
    heads_of_query = query_sequence.astype(jnp.float32).reshape(SEQUENCE_TOKENS, KEY_VALUE_HEADS, QUERY_PER_KEY, HEAD_SIZE)
    heads_of_key = key_sequence.astype(jnp.float32).reshape(SEQUENCE_TOKENS, KEY_VALUE_HEADS, HEAD_SIZE)
    heads_of_value = value_sequence.astype(jnp.float32).reshape(SEQUENCE_TOKENS, KEY_VALUE_HEADS, HEAD_SIZE)
    head_gradients = sequence_output_gradient.astype(jnp.float32).reshape(SEQUENCE_TOKENS, KEY_VALUE_HEADS, QUERY_PER_KEY, HEAD_SIZE)
    scores = jnp.einsum('tjgd,sjd->jgts', heads_of_query, heads_of_key) * scale
    causal = jnp.arange(SEQUENCE_TOKENS)[:, None] >= jnp.arange(SEQUENCE_TOKENS)[None, :]
    scores = jnp.where(causal, scores, -1e+30)
    row_max = lax.optimization_barrier(jnp.max(scores, axis=-1, keepdims=True))
    weight = jnp.exp(scores - row_max)
    probability = weight / lax.optimization_barrier(jnp.sum(weight, axis=-1, keepdims=True))
    prob_low = lax.optimization_barrier(probability.astype(jnp.bfloat16)).astype(jnp.float32)
    value_gradient = jnp.einsum('jgts,tjgd->sjd', prob_low, head_gradients).astype(jnp.bfloat16)
    grad_prob = jnp.einsum('tjgd,sjd->jgts', head_gradients, heads_of_value)
    row_delta = lax.optimization_barrier(jnp.sum(probability * grad_prob, axis=-1, keepdims=True))
    dscore = (probability * (grad_prob - row_delta) * scale).astype(jnp.bfloat16)
    dscore_wide = lax.optimization_barrier(dscore).astype(jnp.float32)
    key_gradient = jnp.einsum('jgts,tjgd->sjd', dscore_wide, heads_of_query).astype(jnp.bfloat16)
    return (key_gradient.reshape(SEQUENCE_TOKENS, KEY_VALUE_HEADS * HEAD_SIZE), value_gradient.reshape(SEQUENCE_TOKENS, KEY_VALUE_HEADS * HEAD_SIZE))

def reference(layer_inputs, norm_gain, queries, output_gradient, w_key, value_matrix, top_grad):
    sequence_count = TOKEN_TOTAL // SEQUENCE_TOKENS
    key_list = []
    value_list = []
    dx_list = []
    for layer_index in range(LAYER_TOTAL):
        wide_inputs = layer_inputs[layer_index].astype(jnp.float32)
        inv_rms = lax.rsqrt(lax.optimization_barrier(jnp.mean(wide_inputs * wide_inputs, axis=-1, keepdims=True)) + epsilon)
        gain_row = norm_gain[layer_index].astype(jnp.float32)
        normed = (wide_inputs * inv_rms * gain_row).astype(jnp.bfloat16)
        key_projected = jnp.dot(normed, w_key[layer_index], preferred_element_type=jnp.float32).astype(jnp.bfloat16)
        value_projected = jnp.dot(normed, value_matrix[layer_index], preferred_element_type=jnp.float32).astype(jnp.bfloat16)
        key_gradient, value_gradient = lax.map(single_sequence, (queries[layer_index].reshape(sequence_count, SEQUENCE_TOKENS, QUERY_HEADS * HEAD_SIZE), key_projected.reshape(sequence_count, SEQUENCE_TOKENS, KEY_VALUE_HEADS * HEAD_SIZE), value_projected.reshape(sequence_count, SEQUENCE_TOKENS, KEY_VALUE_HEADS * HEAD_SIZE), output_gradient[layer_index].reshape(sequence_count, SEQUENCE_TOKENS, QUERY_HEADS * HEAD_SIZE)))
        key_gradient = key_gradient.reshape(TOKEN_TOTAL, KEY_VALUE_HEADS * HEAD_SIZE)
        value_gradient = value_gradient.reshape(TOKEN_TOTAL, KEY_VALUE_HEADS * HEAD_SIZE)
        key_list.append((jnp.dot(normed.T, key_gradient, preferred_element_type=jnp.float32) / N_DP).astype(jnp.bfloat16))
        value_list.append((jnp.dot(normed.T, value_gradient, preferred_element_type=jnp.float32) / N_DP).astype(jnp.bfloat16))
        grad_norm = jnp.dot(key_gradient, w_key[layer_index].T, preferred_element_type=jnp.float32)
        grad_norm = grad_norm + jnp.dot(value_gradient, value_matrix[layer_index].T, preferred_element_type=jnp.float32)
        scaled = gain_row * grad_norm
        layer_dx = inv_rms * scaled - wide_inputs * inv_rms ** 3 * lax.optimization_barrier(jnp.mean(wide_inputs * scaled, axis=-1, keepdims=True))
        dx_list.append(layer_dx)
    carried = top_grad.astype(jnp.float32)
    section_grads = []
    for section_idx in reversed(range(N_SECTION)):
        section_total = carried
        for layer_index in range(section_idx * LAYERS_SECTION, (section_idx + 1) * LAYERS_SECTION):
            section_total = section_total + dx_list[layer_index]
        rounded = section_total.astype(jnp.bfloat16)
        section_grads.insert(0, rounded)
        carried = rounded.astype(jnp.float32)
    return (jnp.stack(key_list), jnp.stack(value_list), jnp.stack(section_grads))
```

```python
import jax
import jax.numpy as jnp
from jax import lax
from jax.sharding import Mesh
from jax.sharding import PartitionSpec as P

HEAD_SIZE = 128
KEY_VALUE_HEADS = 4
SEQUENCE_TOKENS = 128
REPLICAS = 64

epsilon = 1e-05


def normalize(block_inputs, gain_row):
    wide_inputs = block_inputs.astype(jnp.float32)
    inv_rms = lax.rsqrt(jnp.mean(wide_inputs * wide_inputs, axis=-1, keepdims=True) + epsilon)
    return (wide_inputs, inv_rms, (wide_inputs * inv_rms * gain_row).astype(jnp.bfloat16))


def value_pass(heads_of_query, heads_of_key, head_gradients):
    scale = HEAD_SIZE ** (-0.5)
    scores = (
        jnp.einsum(
            "btjgd,bsjd->bjgts", heads_of_query, heads_of_key, preferred_element_type=jnp.float32
        )
        * scale
    )
    causal = lax.broadcasted_iota(
        jnp.int32, (SEQUENCE_TOKENS, SEQUENCE_TOKENS), 0
    ) >= lax.broadcasted_iota(jnp.int32, (SEQUENCE_TOKENS, SEQUENCE_TOKENS), 1)
    scores = jnp.where(causal, scores, -1e30)
    row_max = jnp.max(scores, axis=-1, keepdims=True)
    weight = jnp.exp(scores - row_max)
    probability = weight / jnp.sum(weight, axis=-1, keepdims=True)
    value_gradient = jnp.einsum(
        "bjgts,btjgd->bsjd",
        probability.astype(jnp.bfloat16),
        head_gradients,
        preferred_element_type=jnp.float32,
    )
    return (probability, value_gradient.astype(jnp.bfloat16))


def key_pass(probability, heads_of_query, heads_of_value, head_gradients):
    scale = HEAD_SIZE ** (-0.5)
    grad_prob = jnp.einsum(
        "btjgd,bsjd->bjgts", head_gradients, heads_of_value, preferred_element_type=jnp.float32
    )
    row_delta = jnp.sum(probability * grad_prob, axis=-1, keepdims=True)
    dscore = (probability * (grad_prob - row_delta) * scale).astype(jnp.bfloat16)
    key_gradient = jnp.einsum(
        "bjgts,btjgd->bsjd", dscore, heads_of_query, preferred_element_type=jnp.float32
    )
    return key_gradient.astype(jnp.bfloat16)


def input_term(
    wide_inputs, inv_rms, gain_row, key_gradient, value_gradient, key_weight, value_weight
):
    grad_norm = jnp.einsum(
        "tk,dk->td", key_gradient, key_weight, preferred_element_type=jnp.float32
    )
    grad_norm = grad_norm + jnp.einsum(
        "tk,dk->td", value_gradient, value_weight, preferred_element_type=jnp.float32
    )
    scaled = gain_row * grad_norm
    return inv_rms * scaled - wide_inputs * inv_rms**3 * jnp.mean(
        wide_inputs * scaled, axis=-1, keepdims=True
    )


def ring(value, axis, steps):
    count = lax.axis_size(axis)
    return lax.ppermute(value, axis, [(i, (i + steps) % count) for i in range(count)])


def scatter_sum(parts, axis):
    count = len(parts)
    total = parts[0].astype(jnp.float32)
    received = [ring(parts[k].astype(jnp.bfloat16), axis, k) for k in (1, 3, 2) if k < count]
    for other in received:
        total = total + other.astype(jnp.float32)
    return total


def split(value, axis):
    count = lax.axis_size(axis)
    rows = value.shape[0] // count
    own = lax.axis_index(axis)
    return [
        lax.dynamic_slice_in_dim(value, ((own + k) % count) * rows, rows, 0) for k in range(count)
    ]


def gather(value, axis):
    count = lax.axis_size(axis)
    own = lax.axis_index(axis)
    blocks = [(own, value)]
    for k in (1, 3, 2):
        if k < count:
            blocks.append(((own - k) % count, ring(value, axis, k)))
    return blocks


def place(blocks, rows, base=None, offset=0):
    if base is None:
        total = rows * len(blocks)
        base = jnp.zeros((total,) + blocks[0][1].shape[1:], blocks[0][1].dtype)
    for member, block in blocks:
        base = lax.dynamic_update_slice_in_dim(base, block, offset + member * rows, 0)
    return base


def split_rows(value):
    return value.reshape(2, 64, value.shape[1])


def reduce_first(normed_pair, grad_pair, axis):
    count = lax.axis_size(axis)
    own = lax.axis_index(axis)
    parts = []
    for k in range(count):
        columns = lax.dynamic_slice_in_dim(normed_pair, ((own + k) % count) * 512, 512, 1)
        parts.append(
            jnp.einsum("td,tk->dk", columns, grad_pair, preferred_element_type=jnp.float32)
        )
    return scatter_sum(parts, axis)


def gather_last(piece, axis):
    pieces = gather(piece, axis)
    c = lax.axis_index("c")
    out = jnp.zeros((4096, 512), jnp.bfloat16)
    out = place(pieces, 512, out, c * 2048)
    others = [(member, ring(piece, "c", 1)) for member, piece in pieces]
    return place(others, 512, out, (1 - c) * 2048)


def per_device(layer_inputs, norm_gain, queries, output_gradient, w_key, value_matrix, top_grad):
    is_last = lax.axis_index("s") == 1
    c = lax.axis_index("c")
    block_inputs = layer_inputs[0]
    gain_row = norm_gain[0]
    key_weight = w_key[0]
    value_weight = value_matrix[0]
    wide_inputs, inv_rms, normed = normalize(block_inputs, gain_row)
    own_half = lax.dynamic_slice_in_dim(normed, c * 2048, 2048, 1)
    other_half = ring(lax.dynamic_slice_in_dim(normed, (1 - c) * 2048, 2048, 1), "c", 1)
    normed_pair = jnp.concatenate([own_half, other_half], 0)
    key_projected = jnp.dot(normed, key_weight, preferred_element_type=jnp.float32).astype(
        jnp.bfloat16
    )
    value_projected = jnp.dot(normed, value_weight, preferred_element_type=jnp.float32).astype(
        jnp.bfloat16
    )
    rows = block_inputs.shape[0]
    sequences = rows // SEQUENCE_TOKENS
    heads_of_query = queries[0].reshape(sequences, SEQUENCE_TOKENS, KEY_VALUE_HEADS, -1, HEAD_SIZE)
    head_gradients = output_gradient[0].reshape(
        sequences, SEQUENCE_TOKENS, KEY_VALUE_HEADS, -1, HEAD_SIZE
    )
    heads_of_key = key_projected.reshape(sequences, SEQUENCE_TOKENS, KEY_VALUE_HEADS, HEAD_SIZE)
    heads_of_value = value_projected.reshape(
        sequences, SEQUENCE_TOKENS, KEY_VALUE_HEADS, HEAD_SIZE
    )
    probability, value_gradient = value_pass(heads_of_query, heads_of_key, head_gradients)
    value_gradient = value_gradient.reshape(rows, KEY_VALUE_HEADS * HEAD_SIZE)
    key_gradient = key_pass(probability, heads_of_query, heads_of_value, head_gradients).reshape(
        rows, KEY_VALUE_HEADS * HEAD_SIZE
    )
    value_pair = jnp.concatenate([value_gradient, ring(value_gradient, "c", 1)], 0)
    key_pair = jnp.concatenate([key_gradient, ring(key_gradient, "c", 1)], 0)
    value_part = reduce_first(normed_pair, value_pair, "x")
    key_part = reduce_first(normed_pair, key_pair, "z")
    layer_dx = input_term(
        wide_inputs, inv_rms, gain_row, key_gradient, value_gradient, key_weight, value_weight
    )
    own_total = layer_dx + jnp.where(is_last, top_grad.astype(jnp.float32), 0.0)
    outgoing = own_total.astype(jnp.bfloat16)
    lower, upper = outgoing[:128], outgoing[128:]
    down = [(1, 0)]
    lower_received = lax.ppermute(lower, "s", down)
    value_part = scatter_sum(split(value_part, "z"), "z")
    key_part = scatter_sum(split(key_part, "x"), "x")
    both = jnp.concatenate([split_rows(value_part), split_rows(key_part)], 1)
    own_y = lax.axis_index("y")
    mine = lax.dynamic_index_in_dim(both, own_y, 0, False)
    other = lax.dynamic_index_in_dim(both, 1 - own_y, 0, False)
    mine = mine + ring(other.astype(jnp.bfloat16), "y", 1).astype(jnp.float32)
    block = (mine / REPLICAS).astype(jnp.bfloat16)
    block_other = ring(block, "y", 1)
    first = jnp.where(own_y == 0, block, block_other)
    second = jnp.where(own_y == 0, block_other, block)
    value_block = jnp.concatenate([first[:64], second[:64]], 0)
    key_block = jnp.concatenate([first[64:], second[64:]], 0)
    value_block, upper = lax.optimization_barrier((value_block, upper))
    upper_received = lax.ppermute(upper, "s", down)
    value_piece = place(gather(value_block, "z"), 128)
    key_piece = place(gather(key_block, "x"), 128)
    value_piece, key_piece, own_total, lower_received = lax.optimization_barrier(
        (value_piece, key_piece, own_total, lower_received)
    )
    input_lower = (lower_received.astype(jnp.float32) + own_total[:128]).astype(jnp.bfloat16)
    value_grad = gather_last(value_piece, "x")
    key_grad = gather_last(key_piece, "z")
    value_grad, key_grad, own_total = lax.optimization_barrier((value_grad, key_grad, own_total))
    input_upper = (upper_received.astype(jnp.float32) + own_total[128:]).astype(jnp.bfloat16)
    input_grad = jnp.concatenate([input_lower, input_upper], 0)
    return (key_grad[None], value_grad[None], input_grad[None])


def solution(mesh):
    wide = Mesh(mesh.devices.reshape(2, 4, 4, 2, 2), ("s", "z", "x", "y", "c"))
    dp = ("z", "x", "y", "c")
    in_specs = (
        P("s", dp, None),
        P("s", None),
        P("s", dp, None),
        P("s", dp, None),
        P("s", None, None),
        P("s", None, None),
        P(dp, None),
    )
    out_specs = (P("s", None, None), P("s", None, None), P("s", dp, None))
    return jax.shard_map(
        per_device, mesh=wide, in_specs=in_specs, out_specs=out_specs, check_vma=False
    )
```

```python
import jax
import jax.numpy as jnp
from jax import lax
from jax.experimental import pallas as pl
from jax.experimental.pallas import tpu as pltpu
from jax.sharding import Mesh
from jax.sharding import PartitionSpec as P

HEAD = 128
WIDTH = 4096
COLS = 512
ROWS = 256
REPLICAS = 64
epsilon = 1e-05
SCALE = HEAD ** (-0.5)


bf16 = jnp.bfloat16
f32 = jnp.float32


def shape(dims, dtype):
    return jax.ShapeDtypeStruct(dims, dtype)


def vmem():
    return pl.BlockSpec(memory_space=pltpu.VMEM)


def held(dims, dtype):
    return pltpu.VMEM(dims, dtype)


def hold(*arrays):
    return tuple(pltpu.with_memory_space_constraint(a, pltpu.VMEM) for a in arrays)


def smem():
    return pl.BlockSpec(memory_space=pltpu.SMEM)


def budget(mebibytes):
    return pltpu.CompilerParams(vmem_limit_bytes=mebibytes << 20)


def project_body(place, x, gain, wk, wv, send, mine, keys, values, inverse, acc_k, acc_v, inv):
    step = pl.program_id(0)
    tile = (step + 4 * (1 - place[3])) % 8

    @pl.when(step == 0)
    def _():
        total = jnp.zeros((ROWS, 128), f32)
        for i in range(WIDTH // 128):
            part = x[:, i * 128 : (i + 1) * 128].astype(f32)
            total = total + part * part
        mean = jnp.sum(total, axis=1, keepdims=True) / WIDTH
        inv[...] = jnp.broadcast_to(lax.rsqrt(mean + epsilon), (ROWS, 128))
        inverse[...] = inv[...]
        acc_k[...] = jnp.zeros_like(acc_k)
        acc_v[...] = jnp.zeros_like(acc_v)

    part = x[:, pl.ds(pl.multiple_of(tile * 512, 512), 512)].astype(f32)
    normed = (part * inv[:, :1] * gain[...]).astype(bf16)

    @pl.when(step < 4)
    def _():
        send[...] = normed

    @pl.when(step >= 4)
    def _():
        mine[...] = normed

    acc_k[...] += jnp.dot(normed, wk[...], preferred_element_type=f32)
    acc_v[...] += jnp.dot(normed, wv[...], preferred_element_type=f32)

    @pl.when(step == 7)
    def _():
        keys[...] = acc_k[...]
        values[...] = acc_v[...]


def project(place, x, gain, wk, wv):
    tile = lambda i, p: (i + 4 * (1 - p[3])) % 8
    return pl.pallas_call(
        project_body,
        grid_spec=pltpu.PrefetchScalarGridSpec(
            num_scalar_prefetch=1,
            grid=(8,),
            in_specs=[
                pl.BlockSpec((ROWS, WIDTH), lambda i, p: (0, 0)),
                pl.BlockSpec((1, 512), lambda i, p: (0, tile(i, p))),
                pl.BlockSpec((512, COLS), lambda i, p: (tile(i, p), 0)),
                pl.BlockSpec((512, COLS), lambda i, p: (tile(i, p), 0)),
            ],
            out_specs=[
                pl.BlockSpec((ROWS, 512), lambda i, p: (0, jnp.minimum(i, 3))),
                pl.BlockSpec((ROWS, 512), lambda i, p: (0, jnp.maximum(i - 4, 0))),
                pl.BlockSpec((ROWS, COLS), lambda i, p: (0, 0)),
                pl.BlockSpec((ROWS, COLS), lambda i, p: (0, 0)),
                pl.BlockSpec((ROWS, 128), lambda i, p: (0, 0)),
            ],
            scratch_shapes=[
                pltpu.VMEM((ROWS, COLS), f32),
                pltpu.VMEM((ROWS, COLS), f32),
                pltpu.VMEM((ROWS, 128), f32),
            ],
        ),
        out_shape=[
            shape((ROWS, 2048), bf16),
            shape((ROWS, 2048), bf16),
            shape((ROWS, COLS), f32),
            shape((ROWS, COLS), f32),
            shape((ROWS, 128), f32),
        ],
        cost_estimate=pl.CostEstimate(flops=2 * ROWS * WIDTH * 1024, bytes_accessed=12 << 20, transcendentals=0),
        name="project",
        compiler_params=budget(24),
    )(place, x, gain, wk, wv)


def attend_body(q, og, kf, vf, gk, gv, row):
    def heads(ref):
        return jnp.concatenate([ref[:, h * HEAD : (h + 1) * HEAD] for h in range(4)], axis=0)

    nt = (((1,), (1,)), ((), ()))
    q4 = heads(q)
    g4 = heads(og)
    key = kf[...]
    value = vf[...]
    scores = lax.dot_general(key.astype(bf16), q4, nt, preferred_element_type=f32) * SCALE
    key_at = lax.broadcasted_iota(jnp.int32, (HEAD, 512), 0)
    query_at = lax.broadcasted_iota(jnp.int32, (HEAD, 512), 1) & (HEAD - 1)
    scores = jnp.where(key_at <= query_at, scores, -1e30)
    weight = jnp.exp(scores - jnp.max(scores, axis=0, keepdims=True))
    prob = weight / jnp.sum(weight, axis=0, keepdims=True)
    grad_value = jnp.dot(prob.astype(bf16), g4, preferred_element_type=f32).astype(bf16)
    grad_prob = lax.dot_general(value.astype(bf16), g4, nt, preferred_element_type=f32)
    delta = jnp.sum(prob * grad_prob, axis=0, keepdims=True)
    dscore = (prob * (grad_prob - delta) * SCALE).astype(bf16)
    grad_key = jnp.dot(dscore, q4, preferred_element_type=f32).astype(bf16)
    gk[...] = grad_key
    gv[...] = grad_value
    term = grad_key.astype(f32) * key + grad_value.astype(f32) * value

    @pl.when(pl.program_id(1) == 0)
    def _():
        row[...] = term

    @pl.when(pl.program_id(1) != 0)
    def _():
        row[...] += term


def attend(q, og, kf, vf):
    wide = pl.BlockSpec((128, 512), lambda s, j: (s, j))
    head = pl.BlockSpec((128, 128), lambda s, j: (s, j))
    return pl.pallas_call(
        attend_body,
        grid=(2, 4),
        in_specs=[wide, wide, head, head],
        out_specs=[head, head, pl.BlockSpec((128, 128), lambda s, j: (s, 0))],
        out_shape=[shape((ROWS, COLS), bf16), shape((ROWS, COLS), bf16), shape((ROWS, 128), f32)],
        cost_estimate=pl.CostEstimate(flops=600_000_000 * 4, bytes_accessed=4 << 20, transcendentals=1 << 19),
        name="attend",
        compiler_params=budget(16),
    )(q, og, kf, vf)


def weight_body(place, mine, theirs, grad, grad_theirs, own, *sends, axis):
    tn = (((0,), (0,)), ((), ()))
    for k in (1, 3, 2, 0):
        start = pl.multiple_of(((place[axis] + k) % 4) * 512, 512)
        part = lax.dot_general(
            mine[:, pl.ds(start, 512)], grad[...], tn, preferred_element_type=f32
        ) + lax.dot_general(
            theirs[:, pl.ds(start, 512)], grad_theirs[...], tn, preferred_element_type=f32
        )
        if k == 0:
            own[...] = part
        else:
            sends[k - 1][...] = part.astype(bf16)


def weight_parts(place, mine, theirs, grad, grad_theirs, axis):
    return pl.pallas_call(
        lambda *refs: weight_body(*refs, axis=axis),
        in_specs=[smem()] + [vmem()] * 4,
        out_specs=[vmem()] * 4,
        out_shape=[held((512, COLS), f32)] + [held((512, COLS), bf16)] * 3,
        cost_estimate=pl.CostEstimate(flops=2 * 512 * 2048 * 512, bytes_accessed=5 << 20, transcendentals=0),
        name="weight_parts",
        compiler_params=budget(8),
    )(place, *hold(mine, theirs, grad, grad_theirs))


def input_body(place, gk, gv, wk, wv, x, top, gain, inverse, row, own, lower, upper):
    nt = (((1,), (1,)), ((), ()))
    grad_norm = lax.dot_general(gk[...], wk[...], nt, preferred_element_type=f32)
    grad_norm = grad_norm + lax.dot_general(gv[...], wv[...], nt, preferred_element_type=f32)
    inv = inverse[:, :1]
    mean = jnp.sum(row[...], axis=1, keepdims=True) * (1.0 / WIDTH)
    total = inv * (gain[...] * grad_norm) - x[...].astype(f32) * (inv * inv * mean)
    total = total + jnp.where(place[4] == 1, top[...].astype(f32), 0.0)
    own[...] = total
    low = total.astype(bf16)
    lower[...] = low[:128]
    upper[...] = low[128:]


def input_terms(place, gk, gv, wk, wv, x, top, gain, inverse, row):
    whole = lambda dims: pl.BlockSpec(dims, lambda i, p: (0, 0))
    tile = lambda rows: pl.BlockSpec((rows, 512), lambda i, p: (0, i))
    weight = pl.BlockSpec((512, COLS), lambda i, p: (i, 0))
    return pl.pallas_call(
        input_body,
        grid_spec=pltpu.PrefetchScalarGridSpec(
            num_scalar_prefetch=1,
            grid=(8,),
            in_specs=[
                whole((ROWS, COLS)),
                whole((ROWS, COLS)),
                weight,
                weight,
                tile(ROWS),
                tile(ROWS),
                tile(1),
                whole((ROWS, 128)),
                whole((ROWS, 128)),
            ],
            out_specs=[tile(ROWS), tile(128), tile(128)],
        ),
        out_shape=[shape((ROWS, WIDTH), f32), shape((128, WIDTH), bf16), shape((128, WIDTH), bf16)],
        cost_estimate=pl.CostEstimate(flops=2 * ROWS * WIDTH * 1024, bytes_accessed=18 << 20, transcendentals=0),
        name="input_terms",
        compiler_params=budget(24),
    )(place, gk, gv, wk, wv, x, top, gain, inverse, row)


def finish_body(own, lower, upper, out):
    half = pl.program_id(0)

    @pl.when(half == 0)
    def _():
        out[...] = (lower[...].astype(f32) + own[...]).astype(bf16)

    @pl.when(half == 1)
    def _():
        out[...] = (upper[...].astype(f32) + own[...]).astype(bf16)


def finish(own, lower, upper):
    return pl.pallas_call(
        finish_body,
        grid=(2, 4),
        in_specs=[
            pl.BlockSpec((128, 1024), lambda h, i: (h, i)),
            pl.BlockSpec((128, 1024), lambda h, i: (0, jnp.where(h == 0, i, 3))),
            pl.BlockSpec((128, 1024), lambda h, i: (0, jnp.where(h == 0, 0, i))),
        ],
        out_specs=pl.BlockSpec((128, 1024), lambda h, i: (h, i)),
        out_shape=shape((ROWS, WIDTH), bf16),
        cost_estimate=pl.CostEstimate(flops=ROWS * WIDTH, bytes_accessed=8 << 20, transcendentals=0),
        name="finish",
        compiler_params=budget(8),
    )(own, lower, upper)


def sum_body(place, own, r1, r2, r3, out, *sends, axis):
    for k in (1, 3, 2, 0):
        rows = pl.ds(pl.multiple_of(((place[axis] + k) % 4) * 128, 128), 128)
        part = own[rows, :] + r1[rows, :].astype(f32) + r2[rows, :].astype(f32)
        part = part + r3[rows, :].astype(f32)
        if k == 0:
            out[...] = part
        else:
            sends[k - 1][...] = part.astype(bf16)


def sum_parts(place, own, received, axis):
    return pl.pallas_call(
        lambda *refs: sum_body(*refs, axis=axis),
        in_specs=[smem()] + [vmem()] * 4,
        out_specs=[vmem()] * 4,
        out_shape=[held((128, COLS), f32)] + [held((128, COLS), bf16)] * 3,
        name="sum_parts",
        compiler_params=budget(4),
    )(place, *hold(own, *received))


def pair_body(place, v0, v1, v2, v3, k0, k1, k2, k3, mine, send):
    for at, refs in ((0, (v0, v1, v2, v3)), (64, (k0, k1, k2, k3))):
        for own in (False, True):
            start = (place[2] if own else 1 - place[2]) * 64
            rows = pl.ds(pl.multiple_of(start, 64), 64)
            part = refs[0][rows, :]
            for ref in refs[1:]:
                part = part + ref[rows, :].astype(f32)
            if own:
                mine[at : at + 64, :] = part
            else:
                send[at : at + 64, :] = part.astype(bf16)


def pair_parts(place, value, value_received, key, key_received):
    return pl.pallas_call(
        pair_body,
        in_specs=[smem()] + [vmem()] * 8,
        out_specs=[vmem()] * 2,
        out_shape=[held((128, COLS), f32), held((128, COLS), bf16)],
        name="pair_parts",
        compiler_params=budget(4),
    )(place, *hold(value, *value_received, key, *key_received))


def join_body(place, block, other, value, key):
    for own, ref in ((True, block), (False, other)):
        rows = pl.ds(pl.multiple_of((place[2] if own else 1 - place[2]) * 64, 64), 64)
        value[rows, :] = ref[:64, :]
        key[rows, :] = ref[64:, :]


def join(place, block, other):
    return pl.pallas_call(
        join_body,
        in_specs=[smem()] + [vmem()] * 2,
        out_specs=[vmem()] * 2,
        out_shape=[held((128, COLS), bf16)] * 2,
        name="join",
        compiler_params=budget(4),
    )(place, *hold(block, other))


def stack_body(place, own, r1, r2, r3, out, *, axis):
    for k, ref in enumerate((own, r1, r2, r3)):
        rows = pl.ds(pl.multiple_of(((place[axis] - k + 4) % 4) * 128, 128), 128)
        out[rows, :] = ref[...]


def stack(place, own, received, axis):
    return pl.pallas_call(
        lambda *refs: stack_body(*refs, axis=axis),
        in_specs=[smem()] + [vmem()] * 4,
        out_specs=vmem(),
        out_shape=held((512, COLS), bf16),
        name="stack",
        compiler_params=budget(4),
    )(place, *hold(own, *received))


def assemble(place, value_pieces, key_pieces, value_swapped, key_swapped, ks, start=None):
    groups = []
    for k in ks:
        groups += [(0, k, 0, value_pieces[k]), (1, k, 0, key_pieces[k])]
        groups += [(0, k, 1, value_swapped[k]), (1, k, 1, key_swapped[k])]
    count = len(groups)
    extra = 0 if start is None else 2

    def body(*refs):
        place = refs[0]
        pieces = refs[1 : 1 + count]
        outs = refs[1 + count + extra : 3 + count + extra]
        sems = refs[3 + count + extra]
        copies = []
        for i, (which, k, swapped, _) in enumerate(groups):
            core = (1 - place[3]) if swapped else place[3]
            member = (place[which] - k + 4) % 4
            rows = pl.ds(pl.multiple_of(core * 2048 + member * 512, 512), 512)
            copies.append(pltpu.make_async_copy(pieces[i], outs[which].at[rows, :], sems.at[i]))
        for copy in copies:
            copy.start()
        for copy in copies:
            copy.wait()

    anywhere = pl.BlockSpec(memory_space=pl.ANY)
    return pl.pallas_call(
        body,
        in_specs=[smem()] + [vmem()] * count + [anywhere] * extra,
        out_specs=[anywhere] * 2,
        out_shape=[shape((WIDTH, COLS), bf16)] * 2,
        scratch_shapes=[pltpu.SemaphoreType.DMA((count,))],
        input_output_aliases={} if start is None else {1 + count: 0, 2 + count: 1},
        name="assemble",
        compiler_params=budget(4),
    )(place, *hold(*[g[3] for g in groups]), *(() if start is None else start))


def ring(value, axis, steps):
    count = lax.axis_size(axis)
    return lax.ppermute(value, axis, [(i, (i + steps) % count) for i in range(count)])


def down(value):
    return lax.ppermute(value, "s", [(1, 0)])


def exchange(value_sends, key_sends, value_axis, key_axis):
    value_got, key_got = [None] * 3, [None] * 3
    for k in (1, 3, 2):
        value_got[k - 1] = ring(value_sends[k - 1], value_axis, k)
        key_got[k - 1] = ring(key_sends[k - 1], key_axis, k)
    return value_got, key_got


X, Z = 0, 1


def all_steps(layer_inputs, norm_gain, queries, output_gradient, w_key, value_matrix, top_grad):
    place = jnp.stack([lax.axis_index(a).astype(jnp.int32) for a in ("x", "z", "y", "c", "s")])
    x, wk, wv = layer_inputs[0], w_key[0], value_matrix[0]
    send, mine, keys, values, inverse = project(place, x, norm_gain, wk, wv)
    theirs = ring(send, "c", 1)
    gk, gv, row = attend(queries[0], output_gradient[0], keys, values)
    gv_theirs = ring(gv, "c", 1)
    gk_theirs = ring(gk, "c", 1)
    value_own, *value_sends = weight_parts(place, mine, theirs, gv, gv_theirs, X)
    key_own, *key_sends = weight_parts(place, mine, theirs, gk, gk_theirs, Z)
    value_got, key_got = exchange(value_sends, key_sends, "x", "z")
    own, lower, upper = input_terms(place, gk, gv, wk, wv, x, top_grad, norm_gain, inverse, row)
    lower_got = down(lower)
    value_own, *value_sends = sum_parts(place, value_own, value_got, Z)
    key_own, *key_sends = sum_parts(place, key_own, key_got, X)
    value_got, key_got = exchange(value_sends, key_sends, "z", "x")
    pair, pair_send = pair_parts(place, value_own, value_got, key_own, key_got)
    pair = pair + ring(pair_send, "y", 1).astype(f32)
    block = (pair / REPLICAS).astype(bf16)
    block_other = ring(block, "y", 1)
    value_block, key_block = join(place, block, block_other)
    upper_got = down(upper)
    value_got, key_got = exchange([value_block] * 3, [key_block] * 3, "z", "x")
    value_piece = stack(place, value_block, value_got, Z)
    key_piece = stack(place, key_block, key_got, X)
    value_got, key_got = exchange([value_piece] * 3, [key_piece] * 3, "x", "z")
    value_pieces = [value_piece] + value_got
    key_pieces = [key_piece] + key_got
    value_swapped = [ring(p, "c", 1) for p in value_pieces]
    key_swapped = [ring(p, "c", 1) for p in key_pieces]
    part = assemble(place, value_pieces, key_pieces, value_swapped, key_swapped, (0, 1))
    value_grad, key_grad = assemble(
        place, value_pieces, key_pieces, value_swapped, key_swapped, (3, 2), part
    )
    input_grad = finish(own, lower_got, upper_got)
    return (key_grad[None], value_grad[None], input_grad[None])


def solution(mesh):
    wide = Mesh(mesh.devices.reshape(2, 4, 4, 2, 2), ("s", "z", "x", "y", "c"))
    dp = ("z", "x", "y", "c")
    in_specs = (
        P("s", dp, None),
        P("s", None),
        P("s", dp, None),
        P("s", dp, None),
        P("s", None, None),
        P("s", None, None),
        P(dp, None),
    )
    out_specs = (P("s", None, None), P("s", None, None), P("s", dp, None))
    return jax.shard_map(
        all_steps, mesh=wide, in_specs=in_specs, out_specs=out_specs, check_vma=False
    )
```

```python
import jax
import jax.numpy as jnp
from jax import lax
from jax.experimental import pallas as pl
from jax.experimental.pallas import tpu as pltpu
from jax.sharding import Mesh
from jax.sharding import PartitionSpec as P

HEAD = 128
WIDTH = 4096
COLS = 512
ROWS = 256
REPLICAS = 64
epsilon = 1e-05
SCALE = HEAD ** (-0.5)


bf16 = jnp.bfloat16
f32 = jnp.float32


def shape(dims, dtype):
    return jax.ShapeDtypeStruct(dims, dtype)


def vmem():
    return pl.BlockSpec(memory_space=pltpu.VMEM)


def held(dims, dtype):
    return pltpu.VMEM(dims, dtype)


def hold(*arrays):
    return tuple(pltpu.with_memory_space_constraint(a, pltpu.VMEM) for a in arrays)


def smem():
    return pl.BlockSpec(memory_space=pltpu.SMEM)


def far(*arrays):
    return tuple(pltpu.with_memory_space_constraint(a, pltpu.HBM) for a in arrays)


def budget(mebibytes):
    return pltpu.CompilerParams(vmem_limit_bytes=mebibytes << 20)


def project_body(place, x, gain, wk, wv, send, mine, keys, values, inverse, acc_k, acc_v, inv):
    step = pl.program_id(0)
    tile = (step + 2 * (1 - place[3])) % 4

    @pl.when(step == 0)
    def _():
        total = jnp.zeros((ROWS, 128), f32)
        for i in range(WIDTH // 128):
            part = x[:, i * 128 : (i + 1) * 128].astype(f32)
            total = total + part * part
        mean = jnp.sum(total, axis=1, keepdims=True) / WIDTH
        inv[...] = jnp.broadcast_to(lax.rsqrt(mean + epsilon), (ROWS, 128))
        inverse[...] = inv[...]
        acc_k[...] = jnp.zeros_like(acc_k)
        acc_v[...] = jnp.zeros_like(acc_v)

    part = x[:, pl.ds(pl.multiple_of(tile * 1024, 1024), 1024)].astype(f32)
    normed = (part * inv[:, :1] * gain[...]).astype(bf16)

    @pl.when(step < 2)
    def _():
        send[...] = normed

    @pl.when(step >= 2)
    def _():
        mine[...] = normed

    acc_k[...] += jnp.dot(normed, wk[...], preferred_element_type=f32)
    acc_v[...] += jnp.dot(normed, wv[...], preferred_element_type=f32)

    @pl.when(step == 3)
    def _():
        keys[...] = acc_k[...]
        values[...] = acc_v[...]


def project(place, x, gain, wk, wv):
    tile = lambda i, p: (i + 2 * (1 - p[3])) % 4
    return pl.pallas_call(
        project_body,
        grid_spec=pltpu.PrefetchScalarGridSpec(
            num_scalar_prefetch=1,
            grid=(4,),
            in_specs=[
                pl.BlockSpec((ROWS, WIDTH), lambda i, p: (0, 0)),
                pl.BlockSpec((1, 1024), lambda i, p: (0, tile(i, p))),
                pl.BlockSpec((1024, COLS), lambda i, p: (tile(i, p), 0)),
                pl.BlockSpec((1024, COLS), lambda i, p: (tile(i, p), 0)),
            ],
            out_specs=[
                pl.BlockSpec((ROWS, 1024), lambda i, p: (0, jnp.minimum(i, 1))),
                pl.BlockSpec((ROWS, 1024), lambda i, p: (0, jnp.maximum(i - 2, 0))),
                pl.BlockSpec((ROWS, COLS), lambda i, p: (0, 0)),
                pl.BlockSpec((ROWS, COLS), lambda i, p: (0, 0)),
                pl.BlockSpec((ROWS, 128), lambda i, p: (0, 0)),
            ],
            scratch_shapes=[
                pltpu.VMEM((ROWS, COLS), f32),
                pltpu.VMEM((ROWS, COLS), f32),
                pltpu.VMEM((ROWS, 128), f32),
            ],
        ),
        out_shape=[
            shape((ROWS, 2048), bf16),
            shape((ROWS, 2048), bf16),
            shape((ROWS, COLS), f32),
            shape((ROWS, COLS), f32),
            shape((ROWS, 128), f32),
        ],
        cost_estimate=pl.CostEstimate(flops=2 * ROWS * WIDTH * 1024, bytes_accessed=12 << 20, transcendentals=0),
        name="project",
        compiler_params=budget(24),
    )(place, *far(x), gain, *far(wk, wv))


def attend_body(q, og, kf, vf, gk, gv, row):
    def heads(ref):
        return jnp.concatenate([ref[:, h * HEAD : (h + 1) * HEAD] for h in range(4)], axis=0)

    nt = (((1,), (1,)), ((), ()))
    q4 = heads(q)
    g4 = heads(og)
    key = kf[...]
    value = vf[...]
    scores = lax.dot_general(key.astype(bf16), q4, nt, preferred_element_type=f32) * SCALE
    key_at = lax.broadcasted_iota(jnp.int32, (HEAD, 512), 0)
    query_at = lax.broadcasted_iota(jnp.int32, (HEAD, 512), 1) & (HEAD - 1)
    scores = jnp.where(key_at <= query_at, scores, -1e30)
    weight = jnp.exp(scores - jnp.max(scores, axis=0, keepdims=True))
    prob = weight / jnp.sum(weight, axis=0, keepdims=True)
    grad_value = jnp.dot(prob.astype(bf16), g4, preferred_element_type=f32).astype(bf16)
    grad_prob = lax.dot_general(value.astype(bf16), g4, nt, preferred_element_type=f32)
    delta = jnp.sum(prob * grad_prob, axis=0, keepdims=True)
    dscore = (prob * (grad_prob - delta) * SCALE).astype(bf16)
    grad_key = jnp.dot(dscore, q4, preferred_element_type=f32).astype(bf16)
    gk[...] = grad_key
    gv[...] = grad_value
    term = grad_key.astype(f32) * key + grad_value.astype(f32) * value

    @pl.when(pl.program_id(1) == 0)
    def _():
        row[...] = term

    @pl.when(pl.program_id(1) != 0)
    def _():
        row[...] += term


def attend(q, og, kf, vf):
    wide = pl.BlockSpec((128, 512), lambda s, j: (s, j))
    head = pl.BlockSpec((128, 128), lambda s, j: (s, j))
    return pl.pallas_call(
        attend_body,
        grid=(2, 4),
        in_specs=[wide, wide, head, head],
        out_specs=[head, head, pl.BlockSpec((128, 128), lambda s, j: (s, 0))],
        out_shape=[shape((ROWS, COLS), bf16), shape((ROWS, COLS), bf16), shape((ROWS, 128), f32)],
        cost_estimate=pl.CostEstimate(flops=600_000_000 * 4, bytes_accessed=4 << 20, transcendentals=1 << 19),
        name="attend",
        compiler_params=budget(16),
    )(q, og, kf, vf)


def weight_chunk(place, mine, theirs, grad, grad_theirs, axis, k):
    tn = (((0,), (0,)), ((), ()))
    start = pl.multiple_of(((place[axis] + k) % 4) * 512, 512)
    part = lax.dot_general(mine[:, pl.ds(start, 512)], grad[...], tn, preferred_element_type=f32)
    return part + lax.dot_general(
        theirs[:, pl.ds(start, 512)], grad_theirs[...], tn, preferred_element_type=f32
    )


def weight_far_body(place, mine, theirs, grad, grad_theirs, top, bottom, *, axis):
    part = weight_chunk(place, mine, theirs, grad, grad_theirs, axis, 2).astype(bf16)
    top[...] = part[:256]
    bottom[...] = part[256:]


def weight_far(place, mine, theirs, grad, grad_theirs, axis):
    return pl.pallas_call(
        lambda *refs: weight_far_body(*refs, axis=axis),
        in_specs=[smem()] + [vmem()] * 4,
        out_specs=[vmem()] * 2,
        out_shape=[held((256, COLS), bf16)] * 2,
        cost_estimate=pl.CostEstimate(flops=2 * 512 * 512 * 512, bytes_accessed=2 << 20, transcendentals=0),
        name="weight_far",
        compiler_params=budget(8),
    )(place, *hold(mine, theirs, grad, grad_theirs))


def weight_near_body(place, mine, theirs, grad, grad_theirs, own, ahead, behind, *, axis):
    for k, ref in ((1, ahead), (3, behind), (0, own)):
        ref[...] = weight_chunk(place, mine, theirs, grad, grad_theirs, axis, k)


def weight_near(place, mine, theirs, grad, grad_theirs, axis):
    return pl.pallas_call(
        lambda *refs: weight_near_body(*refs, axis=axis),
        in_specs=[smem()] + [vmem()] * 4,
        out_specs=[vmem()] * 3,
        out_shape=[held((512, COLS), f32)] * 3,
        cost_estimate=pl.CostEstimate(flops=6 * 512 * 512 * 512, bytes_accessed=5 << 20, transcendentals=0),
        name="weight_near",
        compiler_params=budget(8),
    )(place, *hold(mine, theirs, grad, grad_theirs))


def relay_body(ahead, behind, top, bottom, to_ahead, to_behind):
    to_ahead[:256, :] = (ahead[:256, :] + top[...].astype(f32)).astype(bf16)
    to_ahead[256:, :] = ahead[256:, :].astype(bf16)
    to_behind[:256, :] = behind[:256, :].astype(bf16)
    to_behind[256:, :] = (behind[256:, :] + bottom[...].astype(f32)).astype(bf16)


def relay(ahead, behind, top, bottom):
    return pl.pallas_call(
        relay_body,
        in_specs=[vmem()] * 4,
        out_specs=[vmem()] * 2,
        out_shape=[held((512, COLS), bf16)] * 2,
        name="relay",
        compiler_params=budget(4),
    )(*hold(ahead, behind, top, bottom))


def input_body(place, gk, gv, wk, wv, x, top, gain, inverse, row, own, lower, upper):
    nt = (((1,), (1,)), ((), ()))
    grad_norm = lax.dot_general(gk[...], wk[...], nt, preferred_element_type=f32)
    grad_norm = grad_norm + lax.dot_general(gv[...], wv[...], nt, preferred_element_type=f32)
    inv = inverse[:, :1]
    mean = jnp.sum(row[...], axis=1, keepdims=True) * (1.0 / WIDTH)
    total = inv * (gain[...] * grad_norm) - x[...].astype(f32) * (inv * inv * mean)
    total = total + jnp.where(place[4] == 1, top[...].astype(f32), 0.0)
    own[...] = total
    low = total.astype(bf16)
    lower[...] = low[:64]
    upper[...] = low[64:]


def input_terms(place, gk, gv, wk, wv, x, top, gain, inverse, row):
    whole = lambda dims: pl.BlockSpec(dims, lambda i, p: (0, 0))
    tile = lambda rows: pl.BlockSpec((rows, 1024), lambda i, p: (0, i))
    weight = pl.BlockSpec((1024, COLS), lambda i, p: (i, 0))
    return pl.pallas_call(
        input_body,
        grid_spec=pltpu.PrefetchScalarGridSpec(
            num_scalar_prefetch=1,
            grid=(4,),
            in_specs=[
                whole((ROWS, COLS)),
                whole((ROWS, COLS)),
                weight,
                weight,
                tile(ROWS),
                tile(ROWS),
                tile(1),
                whole((ROWS, 128)),
                whole((ROWS, 128)),
            ],
            out_specs=[tile(ROWS), tile(64), tile(192)],
        ),
        out_shape=[shape((ROWS, WIDTH), f32), shape((64, WIDTH), bf16), shape((192, WIDTH), bf16)],
        cost_estimate=pl.CostEstimate(flops=2 * ROWS * WIDTH * 1024, bytes_accessed=18 << 20, transcendentals=0),
        name="input_terms",
        compiler_params=budget(24),
    )(place, gk, gv, wk, wv, x, top, gain, inverse, row)


def finish_body(own, lower, upper, out):
    part = pl.program_id(0)

    @pl.when(part == 0)
    def _():
        out[...] = (lower[...].astype(f32) + own[...]).astype(bf16)

    @pl.when(part != 0)
    def _():
        out[...] = (upper[...].astype(f32) + own[...]).astype(bf16)


def finish(own, lower, upper):
    return pl.pallas_call(
        finish_body,
        grid=(4,),
        in_specs=[
            pl.BlockSpec((64, WIDTH), lambda h: (h, 0)),
            pl.BlockSpec((64, WIDTH), lambda h: (0, 0)),
            pl.BlockSpec((64, WIDTH), lambda h: (jnp.maximum(h - 1, 0), 0)),
        ],
        out_specs=pl.BlockSpec((64, WIDTH), lambda h: (h, 0)),
        out_shape=shape((ROWS, WIDTH), bf16),
        cost_estimate=pl.CostEstimate(flops=ROWS * WIDTH, bytes_accessed=8 << 20, transcendentals=0),
        name="finish",
        compiler_params=budget(12),
    )(own, lower, upper)


def sum_body(place, own, r1, r3, out, *sends, axis):
    for k in (1, 3, 2, 0):
        rows = pl.ds(pl.multiple_of(((place[axis] + k) % 4) * 128, 128), 128)
        part = own[rows, :] + r1[rows, :].astype(f32) + r3[rows, :].astype(f32)
        if k == 0:
            out[...] = part
        else:
            sends[k - 1][...] = part.astype(bf16)


def sum_parts(place, own, r1, r3, axis):
    return pl.pallas_call(
        lambda *refs: sum_body(*refs, axis=axis),
        in_specs=[smem()] + [vmem()] * 3,
        out_specs=[vmem()] * 4,
        out_shape=[held((128, COLS), f32)] + [held((128, COLS), bf16)] * 3,
        name="sum_parts",
        compiler_params=budget(4),
    )(place, *hold(own, r1, r3))


def total_body(own, r1, r2, r3, out):
    part = own[...] + r1[...].astype(f32) + r2[...].astype(f32)
    out[...] = (part + r3[...].astype(f32)).astype(bf16)


def total(own, received):
    return pl.pallas_call(
        total_body,
        in_specs=[vmem()] * 4,
        out_specs=vmem(),
        out_shape=held((128, COLS), bf16),
        name="total",
        compiler_params=budget(4),
    )(*hold(own, *received))


def mean_body(own, other, out):
    out[...] = ((own[...].astype(f32) + other[...].astype(f32)) / REPLICAS).astype(bf16)


def mean(own, other):
    return pl.pallas_call(
        mean_body,
        in_specs=[vmem()] * 2,
        out_specs=vmem(),
        out_shape=held((128, COLS), bf16),
        name="mean",
        compiler_params=budget(4),
    )(*hold(own, other))


def stack_body(place, own, r1, r2, r3, out, *, axis):
    for k, ref in enumerate((own, r1, r2, r3)):
        rows = pl.ds(pl.multiple_of(((place[axis] - k + 4) % 4) * 128, 128), 128)
        out[rows, :] = ref[...]


def stack(place, own, received, axis):
    return pl.pallas_call(
        lambda *refs: stack_body(*refs, axis=axis),
        in_specs=[smem()] + [vmem()] * 4,
        out_specs=vmem(),
        out_shape=held((512, COLS), bf16),
        name="stack",
        compiler_params=budget(4),
    )(place, *hold(own, *received))


def assemble(place, entries, start=None):
    count = len(entries)
    extra = 0 if start is None else 2

    def body(*refs):
        place = refs[0]
        pieces = refs[1 : 1 + count]
        outs = refs[1 + count + extra : 3 + count + extra]
        sems = refs[3 + count + extra]
        copies = []
        for i, (which, k, swapped, first, piece) in enumerate(entries):
            core = (1 - place[3]) if swapped else place[3]
            member = (place[which] - k + 4) % 4
            rows = pl.ds(pl.multiple_of(core * 2048 + member * 512 + first, 256), piece.shape[0])
            copies.append(pltpu.make_async_copy(pieces[i], outs[which].at[rows, :], sems.at[i]))
        for copy in copies:
            copy.start()
        for copy in copies:
            copy.wait()

    anywhere = pl.BlockSpec(memory_space=pl.ANY)
    return pl.pallas_call(
        body,
        in_specs=[smem()] + [vmem()] * count + [anywhere] * extra,
        out_specs=[anywhere] * 2,
        out_shape=[shape((WIDTH, COLS), bf16)] * 2,
        scratch_shapes=[pltpu.SemaphoreType.DMA((count,))],
        input_output_aliases={} if start is None else {1 + count: 0, 2 + count: 1},
        name="assemble",
        compiler_params=budget(4),
    )(place, *hold(*[e[4] for e in entries]), *(() if start is None else start))


def ring(value, axis, steps):
    count = lax.axis_size(axis)
    return lax.ppermute(value, axis, [(i, (i + steps) % count) for i in range(count)])


def down(value):
    return lax.ppermute(value, "s", [(1, 0)])


def send_all(sends, axis):
    got = [None] * 3
    for k in (1, 3, 2):
        got[k - 1] = ring(sends[k - 1], axis, k)
    return got


X, Z = 0, 1


def all_steps(layer_inputs, norm_gain, queries, output_gradient, w_key, value_matrix, top_grad):
    place = jnp.stack([lax.axis_index(a).astype(jnp.int32) for a in ("x", "z", "y", "c", "s")])
    x, wk, wv = layer_inputs[0], w_key[0], value_matrix[0]
    send, mine, keys, values, inverse = project(place, x, norm_gain, wk, wv)
    theirs = ring(send, "c", 1)
    gk, gv, row = attend(queries[0], output_gradient[0], keys, values)
    gv_theirs = ring(gv, "c", 1)
    gk_theirs = ring(gk, "c", 1)
    chains = (
        ("k", (mine, theirs, gk, gk_theirs), Z, X, "z", "x"),
        ("v", (mine, theirs, gv, gv_theirs), X, Z, "x", "z"),
    )
    halves, near, gathered = {}, {}, {}
    for t, operands, first_at, second_at, first, second in chains:
        top, bottom = weight_far(place, *operands, first_at)
        halves[t] = (ring(top, first, 1), ring(bottom, first, 3))
    for t, operands, first_at, second_at, first, second in chains:
        kept, ahead, behind = weight_near(place, *operands, first_at)
        to_ahead, to_behind = relay(ahead, behind, *halves[t])
        near[t] = (kept, ring(to_ahead, first, 1), ring(to_behind, first, 3))
    own, lower, upper = input_terms(place, gk, gv, wk, wv, x, top_grad, norm_gain, inverse, row)
    lower_got = down(lower)
    for t, operands, first_at, second_at, first, second in chains:
        kept, *sends = sum_parts(place, *near[t], second_at)
        got = send_all(sends, second)
        part = total(kept, got)
        block = mean(part, ring(part, "y", 1))
        got = send_all([block] * 3, second)
        piece = stack(place, block, got, second_at)
        behind = ring(piece, first, 1)
        ahead = ring(piece, first, 3)
        top = ring(behind[:256], first, 1)
        bottom = ring(ahead[256:], first, 3)
        which = 1 if t == "k" else 0
        gathered[t] = [
            (which, 0, 0, piece),
            (which, 1, 0, behind),
            (which, 3, 0, ahead),
            (which, 2, 0, top),
            (which, 2, 256, bottom),
        ]
    entries = []
    for at in range(5):
        group = []
        for t in "vk":
            which, k, first_row, block = gathered[t][at]
            group.append((which, k, 0, first_row, block))
            group.append((which, k, 1, first_row, ring(block, "c", 1)))
        entries.append(group)
    upper_got = down(upper)
    part = assemble(place, entries[0])
    part = assemble(place, entries[1] + entries[2], part)
    value_grad, key_grad = assemble(place, entries[3] + entries[4], part)
    input_grad = finish(own, lower_got, upper_got)
    return (key_grad[None], value_grad[None], input_grad[None])


def solution(mesh):
    wide = Mesh(mesh.devices.reshape(2, 4, 4, 2, 2), ("s", "z", "x", "y", "c"))
    dp = ("z", "x", "y", "c")
    in_specs = (
        P("s", dp, None),
        P("s", None),
        P("s", dp, None),
        P("s", dp, None),
        P("s", None, None),
        P("s", None, None),
        P(dp, None),
    )
    out_specs = (P("s", None, None), P("s", None, None), P("s", dp, None))
    return jax.shard_map(all_steps, mesh=wide, in_specs=in_specs, out_specs=out_specs, check_vma=False)
```

```python
import jax
import jax.numpy as jnp
from jax import lax
from jax.experimental import pallas as pl
from jax.experimental.pallas import tpu as pltpu
from jax.sharding import Mesh
from jax.sharding import PartitionSpec as P

HEAD = 128
WIDTH = 4096
COLS = 512
ROWS = 256
REPLICAS = 64
LOWER = 128
epsilon = 1e-05
SCALE = HEAD ** (-0.5)


bf16 = jnp.bfloat16
f32 = jnp.float32


def shape(dims, dtype):
    return jax.ShapeDtypeStruct(dims, dtype)


def vmem():
    return pl.BlockSpec(memory_space=pltpu.VMEM)


def held(dims, dtype):
    return pltpu.VMEM(dims, dtype)


def hold(*arrays):
    return tuple(pltpu.with_memory_space_constraint(a, pltpu.VMEM) for a in arrays)


def held(dims, dtype):
    return pltpu.VMEM(dims, dtype)


def hold(*arrays):
    return tuple(pltpu.with_memory_space_constraint(a, pltpu.VMEM) for a in arrays)


def far(*arrays):
    return tuple(pltpu.with_memory_space_constraint(a, pltpu.HBM) for a in arrays)


def budget(mebibytes):
    return pltpu.CompilerParams(vmem_limit_bytes=mebibytes << 20)


def project_body(x, gain, wk, wv, normed, keys, values, inverse, xs, wks, wvs, sems):
    copies = [
        pltpu.make_async_copy(x.at[pl.ds(64 * i, 64), :], xs.at[pl.ds(64 * i, 64), :], sems.at[i])
        for i in range(4)
    ]
    for i in range(8):
        part = pl.ds(512 * i, 512)
        copies.append(pltpu.make_async_copy(wk.at[part, :], wks.at[part, :], sems.at[4 + 2 * i]))
        copies.append(pltpu.make_async_copy(wv.at[part, :], wvs.at[part, :], sems.at[5 + 2 * i]))
    for copy in copies:
        copy.start()
    for i in range(4):
        copies[i].wait()
        rows = slice(64 * i, 64 * i + 64)
        total = jnp.zeros((64, 128), f32)
        for j in range(WIDTH // 128):
            part = xs[rows, j * 128 : (j + 1) * 128].astype(f32)
            total = total + part * part
        mean = jnp.sum(total, axis=1, keepdims=True) / WIDTH
        inverse[rows, :] = jnp.broadcast_to(lax.rsqrt(mean + epsilon), (64, 128))
    inv = inverse[:, :1]
    for i in range(4):
        for copy in copies[4 + 4 * i : 8 + 4 * i]:
            copy.wait()
        part = slice(1024 * i, 1024 * i + 1024)
        low = (xs[:, part].astype(f32) * inv * gain[:, part]).astype(bf16)
        normed[:, part] = low
        part_k = jnp.dot(low, wks[part, :], preferred_element_type=f32)
        part_v = jnp.dot(low, wvs[part, :], preferred_element_type=f32)
        keys[...] = part_k if i == 0 else keys[...] + part_k
        values[...] = part_v if i == 0 else values[...] + part_v


def project(x, gain, wk, wv):
    anywhere = pl.BlockSpec(memory_space=pl.ANY)
    return pl.pallas_call(
        project_body,
        in_specs=[anywhere, vmem(), anywhere, anywhere],
        out_specs=[vmem()] * 7,
        out_shape=[
            held((ROWS, WIDTH), bf16),
            held((ROWS, COLS), f32),
            held((ROWS, COLS), f32),
            held((ROWS, 128), f32),
            held((ROWS, WIDTH), bf16),
            held((WIDTH, COLS), bf16),
            held((WIDTH, COLS), bf16),
        ],
        scratch_shapes=[pltpu.SemaphoreType.DMA((20,))],
        cost_estimate=pl.CostEstimate(flops=2 * ROWS * WIDTH * 1024, bytes_accessed=12 << 20, transcendentals=0),
        name="project",
        compiler_params=budget(16),
    )(*far(x), *hold(gain), *far(wk, wv))


def attend_body(q, og, kf, vf, gk, gv, keep, send, row):
    first_core = lax.axis_index("c") == 0
    nt = (((1,), (1,)), ((), ()))
    key_at = lax.broadcasted_iota(jnp.int32, (HEAD, 512), 0)
    query_at = lax.broadcasted_iota(jnp.int32, (HEAD, 512), 1) & (HEAD - 1)
    causal = key_at <= query_at
    for s in range(2):
        rows = slice(128 * s, 128 * s + 128)
        terms = None
        for j in range(4):
            columns = slice(HEAD * j, HEAD * j + HEAD)

            def heads(ref):
                first = 512 * j
                return jnp.concatenate(
                    [ref[rows, first + h * HEAD : first + (h + 1) * HEAD] for h in range(4)], axis=0
                )

            q4 = heads(q)
            g4 = heads(og)
            key = kf[rows, columns]
            value = vf[rows, columns]
            scores = lax.dot_general(key.astype(bf16), q4, nt, preferred_element_type=f32) * SCALE
            scores = jnp.where(causal, scores, -1e30)
            weight = jnp.exp(scores - jnp.max(scores, axis=0, keepdims=True))
            prob = weight / jnp.sum(weight, axis=0, keepdims=True)
            grad_value = jnp.dot(prob.astype(bf16), g4, preferred_element_type=f32).astype(bf16)
            grad_prob = lax.dot_general(value.astype(bf16), g4, nt, preferred_element_type=f32)
            delta = jnp.sum(prob * grad_prob, axis=0, keepdims=True)
            dscore = (prob * (grad_prob - delta) * SCALE).astype(bf16)
            grad_key = jnp.dot(dscore, q4, preferred_element_type=f32).astype(bf16)
            gk[rows, columns] = grad_key
            gv[rows, columns] = grad_value
            keep[rows, columns] = jnp.where(first_core, grad_value, grad_key)
            send[rows, columns] = jnp.where(first_core, grad_key, grad_value)
            term = grad_key.astype(f32) * key + grad_value.astype(f32) * value
            terms = term if terms is None else terms + term
        row[rows, :] = terms


def attend(q, og, kf, vf):
    return pl.pallas_call(
        attend_body,
        in_specs=[vmem()] * 4,
        out_specs=[vmem()] * 5,
        out_shape=[held((ROWS, COLS), bf16)] * 4 + [held((ROWS, 128), f32)],
        cost_estimate=pl.CostEstimate(flops=600_000_000 * 4, bytes_accessed=4 << 20, transcendentals=1 << 19),
        name="attend",
        compiler_params=budget(8),
    )(*hold(q, og, kf, vf))


def first_index():
    return jnp.where(lax.axis_index("c") == 0, lax.axis_index("x"), lax.axis_index("z"))


def second_index():
    return jnp.where(lax.axis_index("c") == 0, lax.axis_index("z"), lax.axis_index("x"))


def weight_chunk(mine, theirs, grad, grad_theirs, k):
    tn = (((0,), (0,)), ((), ()))
    start = pl.multiple_of(((first_index() + k) % 4) * 1024, 1024)
    part = lax.dot_general(mine[:, pl.ds(start, 1024)], grad[...], tn, preferred_element_type=f32)
    return part + lax.dot_general(
        theirs[:, pl.ds(start, 1024)], grad_theirs[...], tn, preferred_element_type=f32
    )


def weight_far_body(mine, theirs, grad, grad_theirs, top, bottom):
    part = weight_chunk(mine, theirs, grad, grad_theirs, 2).astype(bf16)
    top[...] = part[:512]
    bottom[...] = part[512:]


def weight_far(mine, theirs, grad, grad_theirs):
    return pl.pallas_call(
        weight_far_body,
        in_specs=[vmem()] * 4,
        out_specs=[vmem()] * 2,
        out_shape=[held((512, COLS), bf16)] * 2,
        cost_estimate=pl.CostEstimate(flops=4 * 512 * 512 * 512, bytes_accessed=2 << 20, transcendentals=0),
        name="weight_far",
        compiler_params=budget(8),
    )(*hold(mine, theirs, grad, grad_theirs))


def weight_near_body(mine, theirs, grad, grad_theirs, a_top, a_bottom, b_top, b_bottom):
    part = weight_chunk(mine, theirs, grad, grad_theirs, 1)
    a_top[...] = part[:512]
    a_bottom[...] = part[512:].astype(bf16)
    part = weight_chunk(mine, theirs, grad, grad_theirs, 3)
    b_top[...] = part[:512].astype(bf16)
    b_bottom[...] = part[512:]


def weight_near(mine, theirs, grad, grad_theirs):
    return pl.pallas_call(
        weight_near_body,
        in_specs=[vmem()] * 4,
        out_specs=[vmem()] * 4,
        out_shape=[
            held((512, COLS), f32),
            held((512, COLS), bf16),
            held((512, COLS), bf16),
            held((512, COLS), f32),
        ],
        cost_estimate=pl.CostEstimate(flops=8 * 512 * 512 * 512, bytes_accessed=5 << 20, transcendentals=0),
        name="weight_near",
        compiler_params=budget(12),
    )(*hold(mine, theirs, grad, grad_theirs))


def weight_own_body(mine, theirs, grad, grad_theirs, own):
    own[...] = weight_chunk(mine, theirs, grad, grad_theirs, 0)


def weight_own(mine, theirs, grad, grad_theirs):
    return pl.pallas_call(
        weight_own_body,
        in_specs=[vmem()] * 4,
        out_specs=vmem(),
        out_shape=held((1024, COLS), f32),
        cost_estimate=pl.CostEstimate(flops=4 * 512 * 512 * 512, bytes_accessed=5 << 20, transcendentals=0),
        name="weight_own",
        compiler_params=budget(8),
    )(*hold(mine, theirs, grad, grad_theirs))


def relay_body(own, arrived, out):
    out[...] = (own[...] + arrived[...].astype(f32)).astype(bf16)


def relay(own, arrived):
    return pl.pallas_call(
        relay_body,
        in_specs=[vmem()] * 2,
        out_specs=vmem(),
        out_shape=held((512, COLS), bf16),
        name="relay",
        compiler_params=budget(4),
    )(*hold(own, arrived))


def input_body(gk, gv, wk, wv, x, top, gain, inverse, row, own, lower, upper):
    nt = (((1,), (1,)), ((), ()))
    inv = inverse[:, :1]
    mean = jnp.sum(row[...], axis=1, keepdims=True) * (1.0 / WIDTH)
    factor = inv * inv * mean
    last = lax.axis_index("s") == 1
    for i in range(8):
        tile = slice(512 * i, 512 * i + 512)
        grad_norm = lax.dot_general(gk[...], wk[tile, :], nt, preferred_element_type=f32)
        grad_norm = grad_norm + lax.dot_general(
            gv[...], wv[tile, :], nt, preferred_element_type=f32
        )
        total = inv * (gain[:, tile] * grad_norm) - x[:, tile].astype(f32) * factor
        total = total + jnp.where(last, top[:, tile].astype(f32), 0.0)
        own[:, tile] = total
        low = total.astype(bf16)
        lower[:, tile] = low[:LOWER]
        upper[:, tile] = low[LOWER:]


def input_terms(gk, gv, wk, wv, x, top, gain, inverse, row):
    return pl.pallas_call(
        input_body,
        in_specs=[vmem()] * 9,
        out_specs=[vmem()] * 3,
        out_shape=[held((ROWS, WIDTH), f32), held((LOWER, WIDTH), bf16), held((ROWS - LOWER, WIDTH), bf16)],
        cost_estimate=pl.CostEstimate(flops=2 * ROWS * WIDTH * 1024, bytes_accessed=18 << 20, transcendentals=0),
        name="input_terms",
        compiler_params=budget(8),
    )(*hold(gk, gv, wk, wv, x, top, gain, inverse, row))


def finish_body(own, lower, upper, out, buffer, sems):
    copies = []
    for i in range(ROWS // 32):
        rows = slice(32 * i, 32 * i + 32)
        if 32 * i < LOWER:
            received = lower[rows, :]
        else:
            received = upper[32 * i - LOWER : 32 * i - LOWER + 32, :]
        buffer[rows, :] = (received.astype(f32) + own[rows, :]).astype(bf16)
        part = pl.ds(32 * i, 32)
        copies.append(pltpu.make_async_copy(buffer.at[part, :], out.at[part, :], sems.at[i]))
        copies[-1].start()
    for copy in copies:
        copy.wait()


def finish(own, lower, upper):
    return pl.pallas_call(
        finish_body,
        in_specs=[vmem()] * 3,
        out_specs=pl.BlockSpec(memory_space=pl.ANY),
        out_shape=shape((ROWS, WIDTH), bf16),
        scratch_shapes=[pltpu.VMEM((ROWS, WIDTH), bf16), pltpu.SemaphoreType.DMA((ROWS // 32,))],
        cost_estimate=pl.CostEstimate(flops=ROWS * WIDTH, bytes_accessed=8 << 20, transcendentals=0),
        name="finish",
        compiler_params=budget(8),
    )(*hold(own, lower, upper))


def sum_body(own, b_top, b_bottom, a_top, a_bottom, out, s1, s2, s3, whole):
    whole[:512] = own[:512] + b_top[...].astype(f32) + a_top[...].astype(f32)
    whole[512:] = own[512:] + b_bottom[...].astype(f32) + a_bottom[...].astype(f32)
    for k, ref in ((1, s1), (3, s3), (2, s2), (0, out)):
        rows = pl.ds(pl.multiple_of(((second_index() + k) % 4) * 256, 256), 256)
        ref[...] = whole[rows, :].astype(ref.dtype)


def sum_parts(own, *halves):
    return pl.pallas_call(
        sum_body,
        in_specs=[vmem()] * 5,
        out_specs=[vmem()] * 4,
        out_shape=[held((256, COLS), f32)] + [held((256, COLS), bf16)] * 3,
        scratch_shapes=[pltpu.VMEM((1024, COLS), f32)],
        name="sum_parts",
        compiler_params=budget(8),
    )(*hold(own, *halves))


def total_body(own, r1, r2, r3, out):
    part = own[...] + r1[...].astype(f32) + r2[...].astype(f32)
    out[...] = (part + r3[...].astype(f32)).astype(bf16)


def total(own, received):
    return pl.pallas_call(
        total_body,
        in_specs=[vmem()] * 4,
        out_specs=vmem(),
        out_shape=held((256, COLS), bf16),
        name="total",
        compiler_params=budget(4),
    )(*hold(own, *received))


def mean_body(own, other, out):
    out[...] = ((own[...].astype(f32) + other[...].astype(f32)) / REPLICAS).astype(bf16)


def mean(own, other):
    return pl.pallas_call(
        mean_body,
        in_specs=[vmem()] * 2,
        out_specs=vmem(),
        out_shape=held((256, COLS), bf16),
        name="mean",
        compiler_params=budget(4),
    )(*hold(own, other))


def stack_body(own, r1, r2, r3, top, bottom, whole):
    for k, ref in enumerate((own, r1, r2, r3)):
        rows = pl.ds(pl.multiple_of(((second_index() - k + 4) % 4) * 256, 256), 256)
        whole[rows, :] = ref[...]
    top[...] = whole[:512]
    bottom[...] = whole[512:]


def stack(own, received):
    return pl.pallas_call(
        stack_body,
        in_specs=[vmem()] * 4,
        out_specs=[vmem()] * 2,
        out_shape=[held((512, COLS), bf16)] * 2,
        scratch_shapes=[pltpu.VMEM((1024, COLS), bf16)],
        name="stack",
        compiler_params=budget(4),
    )(*hold(own, *received))


def assemble(entries, start=None):
    count = len(entries)
    extra = 0 if start is None else 2

    def body(*refs):
        core = lax.axis_index("c")
        owners = (lax.axis_index("x"), lax.axis_index("z"))
        pieces = refs[: 2 * count]
        outs = refs[2 * count + extra : 2 * count + extra + 2]
        sems = refs[2 * count + extra + 2]

        def copies(which):
            made = []
            for i, (k, first, own, _) in enumerate(entries):
                for at, gradient in ((2 * i, which), (2 * i + 1, 1 - which)):
                    member = (owners[gradient] - k + 4) % 4
                    rows = pl.ds(pl.multiple_of(member * 1024 + first, 512), own.shape[0])
                    made.append(
                        pltpu.make_async_copy(pieces[at], outs[gradient].at[rows, :], sems.at[at])
                    )
            return made

        for which in (0, 1):

            @pl.when(core == which)
            def _():
                made = copies(which)
                for copy in made:
                    copy.start()
                for copy in made:
                    copy.wait()

    anywhere = pl.BlockSpec(memory_space=pl.ANY)
    blocks = [block for entry in entries for block in entry[2:]]
    return pl.pallas_call(
        body,
        in_specs=[vmem()] * (2 * count) + [anywhere] * extra,
        out_specs=[anywhere] * 2,
        out_shape=[shape((WIDTH, COLS), bf16)] * 2,
        scratch_shapes=[pltpu.SemaphoreType.DMA((2 * count,))],
        input_output_aliases={} if start is None else {2 * count: 0, 2 * count + 1: 1},
        name="assemble",
        compiler_params=budget(4),
    )(*hold(*blocks), *(() if start is None else start))


def swap(value, axis):
    return lax.ppermute(value, axis, [(0, 1), (1, 0)])


def ring(value, stage, steps):
    pairs = []
    for z in range(4):
        for x in range(4):
            for c in range(2):
                along_x = (c == 0) == (stage == 1)
                to = (z, (x + steps) % 4) if along_x else ((z + steps) % 4, x)
                pairs.append(((z * 4 + x) * 2 + c, (to[0] * 4 + to[1]) * 2 + c))
    return lax.ppermute(value, ("z", "x", "c"), pairs)


def down(value):
    return lax.ppermute(value, "s", [(1, 0)])


def send_all(sends, stage):
    got = [None] * 3
    for k in (1, 3, 2):
        got[k - 1] = ring(sends[k - 1], stage, k)
    return got


def all_steps(layer_inputs, norm_gain, queries, output_gradient, w_key, value_matrix, top_grad):
    x, wk, wv = layer_inputs[0], w_key[0], value_matrix[0]
    normed, keys, values, inverse, x, wk, wv = project(x, norm_gain, wk, wv)
    theirs = swap(normed, "c")
    gk, gv, keep, send, row = attend(queries[0], output_gradient[0], keys, values)
    operands = (normed, theirs, keep, swap(send, "c"))
    top, bottom = weight_far(*operands)
    top, bottom = ring(top, 1, 1), ring(bottom, 1, 3)
    a_top, a_bottom, b_top, b_bottom = weight_near(*operands)
    from_bottom, from_top = ring(a_bottom, 1, 1), ring(b_top, 1, 3)
    kept = weight_own(*operands)
    a_top, b_bottom = relay(a_top, top), relay(b_bottom, bottom)
    halves = (ring(a_top, 1, 1), from_bottom, from_top, ring(b_bottom, 1, 3))
    own, lower, upper = input_terms(gk, gv, wk, wv, x, top_grad, norm_gain, inverse, row)
    lower_got = down(lower)
    kept, *sends = sum_parts(kept, *halves)
    got = send_all(sends, 2)
    part = total(kept, got)
    block = mean(part, swap(part, "y"))
    upper_got = down(upper)
    got = send_all([block] * 3, 2)
    top, bottom = stack(block, got)
    behind_top, ahead_bottom = ring(top, 1, 1), ring(bottom, 1, 3)
    behind_bottom, ahead_top = ring(bottom, 1, 1), ring(top, 1, 3)
    blocks = (
        (0, 0, top),
        (0, 512, bottom),
        (1, 0, behind_top),
        (3, 512, ahead_bottom),
        (1, 512, behind_bottom),
        (3, 0, ahead_top),
        (2, 0, ring(behind_top, 1, 1)),
        (2, 512, ring(ahead_bottom, 1, 3)),
    )
    entries = [(k, first, block, swap(block, "c")) for k, first, block in blocks]
    part = assemble(entries[:2])
    part = assemble(entries[2:4], part)
    part = assemble(entries[4:6], part)
    value_grad, key_grad = assemble(entries[6:], part)
    input_grad = finish(own, lower_got, upper_got)
    return (key_grad[None], value_grad[None], input_grad[None])


def solution(mesh):
    wide = Mesh(mesh.devices.reshape(2, 4, 4, 2, 2), ("s", "z", "x", "y", "c"))
    dp = ("z", "x", "y", "c")
    in_specs = (
        P("s", dp, None),
        P("s", None),
        P("s", dp, None),
        P("s", dp, None),
        P("s", None, None),
        P("s", None, None),
        P(dp, None),
    )
    out_specs = (P("s", None, None), P("s", None, None), P("s", dp, None))
    return jax.shard_map(all_steps, mesh=wide, in_specs=in_specs, out_specs=out_specs, check_vma=False)
```

```python
import jax
import jax.numpy as jnp
from jax import lax
from jax.experimental import pallas as pl
from jax.experimental.pallas import tpu as pltpu
from jax.sharding import Mesh
from jax.sharding import PartitionSpec as P

HEAD = 128
WIDTH = 4096
COLS = 512
ROWS = 256
REPLICAS = 64
LOWER = 128
epsilon = 1e-05
SCALE = HEAD ** (-0.5)


bf16 = jnp.bfloat16
f32 = jnp.float32


def shape(dims, dtype):
    return jax.ShapeDtypeStruct(dims, dtype)


def vmem():
    return pl.BlockSpec(memory_space=pltpu.VMEM)


def held(dims, dtype):
    return pltpu.VMEM(dims, dtype)


def hold(*arrays):
    return tuple(pltpu.with_memory_space_constraint(a, pltpu.VMEM) for a in arrays)


def held(dims, dtype):
    return pltpu.VMEM(dims, dtype)


def hold(*arrays):
    return tuple(pltpu.with_memory_space_constraint(a, pltpu.VMEM) for a in arrays)


def far(*arrays):
    return tuple(pltpu.with_memory_space_constraint(a, pltpu.HBM) for a in arrays)


def budget(mebibytes):
    return pltpu.CompilerParams(vmem_limit_bytes=mebibytes << 20)


def project_body(x, gain_row, wk, wv, normed, keys, values, inverse, xs, wks, wvs, gain, sems):
    copies = [
        pltpu.make_async_copy(x.at[pl.ds(64 * i, 64), :], xs.at[pl.ds(64 * i, 64), :], sems.at[i])
        for i in range(4)
    ]
    for i in range(8):
        part = pl.ds(512 * i, 512)
        copies.append(pltpu.make_async_copy(wk.at[part, :], wks.at[part, :], sems.at[4 + 2 * i]))
        copies.append(pltpu.make_async_copy(wv.at[part, :], wvs.at[part, :], sems.at[5 + 2 * i]))
    gain_copy = pltpu.make_async_copy(gain_row, gain, sems.at[20])
    gain_copy.start()
    for copy in copies:
        copy.start()
    gain_copy.wait()
    for i in range(4):
        copies[i].wait()
        rows = slice(64 * i, 64 * i + 64)
        total = jnp.zeros((64, 128), f32)
        for j in range(WIDTH // 128):
            part = xs[rows, j * 128 : (j + 1) * 128].astype(f32)
            total = total + part * part
        mean = jnp.sum(total, axis=1, keepdims=True) / WIDTH
        inverse[rows, :] = jnp.broadcast_to(lax.rsqrt(mean + epsilon), (64, 128))
    inv = inverse[:, :1]
    for i in range(4):
        for copy in copies[4 + 4 * i : 8 + 4 * i]:
            copy.wait()
        part = slice(1024 * i, 1024 * i + 1024)
        low = (xs[:, part].astype(f32) * inv * gain[:, part]).astype(bf16)
        normed[:, part] = low
        part_k = jnp.dot(low, wks[part, :], preferred_element_type=f32)
        part_v = jnp.dot(low, wvs[part, :], preferred_element_type=f32)
        keys[...] = part_k if i == 0 else keys[...] + part_k
        values[...] = part_v if i == 0 else values[...] + part_v


def project(x, gain, wk, wv):
    anywhere = pl.BlockSpec(memory_space=pl.ANY)
    return pl.pallas_call(
        project_body,
        in_specs=[anywhere] * 4,
        out_specs=[vmem()] * 7,
        out_shape=[
            held((ROWS, WIDTH), bf16),
            held((ROWS, COLS), f32),
            held((ROWS, COLS), f32),
            held((ROWS, 128), f32),
            held((ROWS, WIDTH), bf16),
            held((WIDTH, COLS), bf16),
            held((WIDTH, COLS), bf16),
        ],
        scratch_shapes=[pltpu.VMEM((1, WIDTH), f32), pltpu.SemaphoreType.DMA((21,))],
        cost_estimate=pl.CostEstimate(flops=2 * ROWS * WIDTH * 1024, bytes_accessed=12 << 20, transcendentals=0),
        name="project",
        compiler_params=budget(16),
    )(*far(x, gain, wk, wv))


def attend_body(q, og, kf, vf, gk, gv, keep, send, row):
    first_core = lax.axis_index("c") == 0
    nt = (((1,), (1,)), ((), ()))
    key_at = lax.broadcasted_iota(jnp.int32, (HEAD, 512), 0)
    query_at = lax.broadcasted_iota(jnp.int32, (HEAD, 512), 1) & (HEAD - 1)
    causal = key_at <= query_at
    for s in range(2):
        rows = slice(128 * s, 128 * s + 128)
        terms = None
        for j in range(4):
            columns = slice(HEAD * j, HEAD * j + HEAD)

            def heads(ref):
                first = 512 * j
                return jnp.concatenate(
                    [ref[rows, first + h * HEAD : first + (h + 1) * HEAD] for h in range(4)], axis=0
                )

            q4 = heads(q)
            g4 = heads(og)
            key = kf[rows, columns]
            value = vf[rows, columns]
            scores = lax.dot_general(key.astype(bf16), q4, nt, preferred_element_type=f32) * SCALE
            scores = jnp.where(causal, scores, -1e30)
            weight = jnp.exp(scores - jnp.max(scores, axis=0, keepdims=True))
            prob = weight / jnp.sum(weight, axis=0, keepdims=True)
            grad_value = jnp.dot(prob.astype(bf16), g4, preferred_element_type=f32).astype(bf16)
            grad_prob = lax.dot_general(value.astype(bf16), g4, nt, preferred_element_type=f32)
            delta = jnp.sum(prob * grad_prob, axis=0, keepdims=True)
            dscore = (prob * (grad_prob - delta) * SCALE).astype(bf16)
            grad_key = jnp.dot(dscore, q4, preferred_element_type=f32).astype(bf16)
            gk[rows, columns] = grad_key
            gv[rows, columns] = grad_value
            keep[rows, columns] = jnp.where(first_core, grad_value, grad_key)
            send[rows, columns] = jnp.where(first_core, grad_key, grad_value)
            term = grad_key.astype(f32) * key + grad_value.astype(f32) * value
            terms = term if terms is None else terms + term
        row[rows, :] = terms


def attend(q, og, kf, vf):
    return pl.pallas_call(
        attend_body,
        in_specs=[vmem()] * 4,
        out_specs=[vmem()] * 5,
        out_shape=[held((ROWS, COLS), bf16)] * 4 + [held((ROWS, 128), f32)],
        cost_estimate=pl.CostEstimate(flops=600_000_000 * 4, bytes_accessed=4 << 20, transcendentals=1 << 19),
        name="attend",
        compiler_params=budget(8),
    )(*hold(q, og, kf, vf))


def first_index():
    return jnp.where(lax.axis_index("c") == 0, lax.axis_index("x"), lax.axis_index("z"))


def second_index():
    return jnp.where(lax.axis_index("c") == 0, lax.axis_index("z"), lax.axis_index("x"))


def weight_chunk(mine, theirs, grad, grad_theirs, k):
    tn = (((0,), (0,)), ((), ()))
    start = pl.multiple_of(((first_index() + k) % 4) * 1024, 1024)
    part = lax.dot_general(mine[:, pl.ds(start, 1024)], grad[...], tn, preferred_element_type=f32)
    return part + lax.dot_general(
        theirs[:, pl.ds(start, 1024)], grad_theirs[...], tn, preferred_element_type=f32
    )


def weight_far_body(mine, theirs, grad, grad_theirs, top, bottom):
    part = weight_chunk(mine, theirs, grad, grad_theirs, 2).astype(bf16)
    top[...] = part[:512]
    bottom[...] = part[512:]


def weight_far(mine, theirs, grad, grad_theirs):
    return pl.pallas_call(
        weight_far_body,
        in_specs=[vmem()] * 4,
        out_specs=[vmem()] * 2,
        out_shape=[held((512, COLS), bf16)] * 2,
        cost_estimate=pl.CostEstimate(flops=4 * 512 * 512 * 512, bytes_accessed=2 << 20, transcendentals=0),
        name="weight_far",
        compiler_params=budget(8),
    )(*hold(mine, theirs, grad, grad_theirs))


def weight_near_body(mine, theirs, grad, grad_theirs, a_top, a_bottom, b_top, b_bottom):
    part = weight_chunk(mine, theirs, grad, grad_theirs, 1)
    a_top[...] = part[:512]
    a_bottom[...] = part[512:].astype(bf16)
    part = weight_chunk(mine, theirs, grad, grad_theirs, 3)
    b_top[...] = part[:512].astype(bf16)
    b_bottom[...] = part[512:]


def weight_near(mine, theirs, grad, grad_theirs):
    return pl.pallas_call(
        weight_near_body,
        in_specs=[vmem()] * 4,
        out_specs=[vmem()] * 4,
        out_shape=[
            held((512, COLS), f32),
            held((512, COLS), bf16),
            held((512, COLS), bf16),
            held((512, COLS), f32),
        ],
        cost_estimate=pl.CostEstimate(flops=8 * 512 * 512 * 512, bytes_accessed=5 << 20, transcendentals=0),
        name="weight_near",
        compiler_params=budget(12),
    )(*hold(mine, theirs, grad, grad_theirs))


def weight_own_body(mine, theirs, grad, grad_theirs, own):
    own[...] = weight_chunk(mine, theirs, grad, grad_theirs, 0)


def weight_own(mine, theirs, grad, grad_theirs):
    return pl.pallas_call(
        weight_own_body,
        in_specs=[vmem()] * 4,
        out_specs=vmem(),
        out_shape=held((1024, COLS), f32),
        cost_estimate=pl.CostEstimate(flops=4 * 512 * 512 * 512, bytes_accessed=5 << 20, transcendentals=0),
        name="weight_own",
        compiler_params=budget(8),
    )(*hold(mine, theirs, grad, grad_theirs))


def relay_body(own, arrived, out):
    out[...] = (own[...] + arrived[...].astype(f32)).astype(bf16)


def relay(own, arrived):
    return pl.pallas_call(
        relay_body,
        in_specs=[vmem()] * 2,
        out_specs=vmem(),
        out_shape=held((512, COLS), bf16),
        name="relay",
        compiler_params=budget(4),
    )(*hold(own, arrived))


def input_body(gk, gv, wk, wv, x, top, gain, inverse, row, own, lower, upper):
    nt = (((1,), (1,)), ((), ()))
    inv = inverse[:, :1]
    mean = jnp.sum(row[...], axis=1, keepdims=True) * (1.0 / WIDTH)
    factor = inv * inv * mean
    last = lax.axis_index("s") == 1
    for i in range(8):
        tile = slice(512 * i, 512 * i + 512)
        grad_norm = lax.dot_general(gk[...], wk[tile, :], nt, preferred_element_type=f32)
        grad_norm = grad_norm + lax.dot_general(
            gv[...], wv[tile, :], nt, preferred_element_type=f32
        )
        total = inv * (gain[:, tile] * grad_norm) - x[:, tile].astype(f32) * factor
        total = total + jnp.where(last, top[:, tile].astype(f32), 0.0)
        own[:, tile] = total
        low = total.astype(bf16)
        lower[:, tile] = low[:LOWER]
        upper[:, tile] = low[LOWER:]


def input_terms(gk, gv, wk, wv, x, top, gain, inverse, row):
    return pl.pallas_call(
        input_body,
        in_specs=[vmem()] * 9,
        out_specs=[vmem()] * 3,
        out_shape=[held((ROWS, WIDTH), f32), held((LOWER, WIDTH), bf16), held((ROWS - LOWER, WIDTH), bf16)],
        cost_estimate=pl.CostEstimate(flops=2 * ROWS * WIDTH * 1024, bytes_accessed=18 << 20, transcendentals=0),
        name="input_terms",
        compiler_params=budget(8),
    )(*hold(gk, gv, wk, wv, x, top, gain, inverse, row))


def finish_body(own, lower, upper, out, buffer, sems):
    copies = []
    for i in range(ROWS // 32):
        rows = slice(32 * i, 32 * i + 32)
        if 32 * i < LOWER:
            received = lower[rows, :]
        else:
            received = upper[32 * i - LOWER : 32 * i - LOWER + 32, :]
        buffer[rows, :] = (received.astype(f32) + own[rows, :]).astype(bf16)
        part = pl.ds(32 * i, 32)
        copies.append(pltpu.make_async_copy(buffer.at[part, :], out.at[part, :], sems.at[i]))
        copies[-1].start()
    for copy in copies:
        copy.wait()


def finish(own, lower, upper):
    return pl.pallas_call(
        finish_body,
        in_specs=[vmem()] * 3,
        out_specs=pl.BlockSpec(memory_space=pl.ANY),
        out_shape=shape((ROWS, WIDTH), bf16),
        scratch_shapes=[pltpu.VMEM((ROWS, WIDTH), bf16), pltpu.SemaphoreType.DMA((ROWS // 32,))],
        cost_estimate=pl.CostEstimate(flops=ROWS * WIDTH, bytes_accessed=8 << 20, transcendentals=0),
        name="finish",
        compiler_params=budget(8),
    )(*hold(own, lower, upper))


def sum_body(own, b_top, b_bottom, a_top, a_bottom, out, s1, s2, s3, whole):
    whole[:512] = own[:512] + b_top[...].astype(f32) + a_top[...].astype(f32)
    whole[512:] = own[512:] + b_bottom[...].astype(f32) + a_bottom[...].astype(f32)
    for k, ref in ((1, s1), (3, s3), (2, s2), (0, out)):
        rows = pl.ds(pl.multiple_of(((second_index() + k) % 4) * 256, 256), 256)
        ref[...] = whole[rows, :].astype(ref.dtype)


def sum_parts(own, *halves):
    return pl.pallas_call(
        sum_body,
        in_specs=[vmem()] * 5,
        out_specs=[vmem()] * 4,
        out_shape=[held((256, COLS), f32)] + [held((256, COLS), bf16)] * 3,
        scratch_shapes=[pltpu.VMEM((1024, COLS), f32)],
        name="sum_parts",
        compiler_params=budget(8),
    )(*hold(own, *halves))


def total_body(own, r1, r2, r3, out):
    part = own[...] + r1[...].astype(f32) + r2[...].astype(f32)
    out[...] = (part + r3[...].astype(f32)).astype(bf16)


def total(own, received):
    return pl.pallas_call(
        total_body,
        in_specs=[vmem()] * 4,
        out_specs=vmem(),
        out_shape=held((256, COLS), bf16),
        name="total",
        compiler_params=budget(4),
    )(*hold(own, *received))


def mean_body(own, other, out):
    out[...] = ((own[...].astype(f32) + other[...].astype(f32)) / REPLICAS).astype(bf16)


def mean(own, other):
    return pl.pallas_call(
        mean_body,
        in_specs=[vmem()] * 2,
        out_specs=vmem(),
        out_shape=held((256, COLS), bf16),
        name="mean",
        compiler_params=budget(4),
    )(*hold(own, other))


def stack_body(own, r1, r2, r3, top, bottom, whole):
    for k, ref in enumerate((own, r1, r2, r3)):
        rows = pl.ds(pl.multiple_of(((second_index() - k + 4) % 4) * 256, 256), 256)
        whole[rows, :] = ref[...]
    top[...] = whole[:512]
    bottom[...] = whole[512:]


def stack(own, received):
    return pl.pallas_call(
        stack_body,
        in_specs=[vmem()] * 4,
        out_specs=[vmem()] * 2,
        out_shape=[held((512, COLS), bf16)] * 2,
        scratch_shapes=[pltpu.VMEM((1024, COLS), bf16)],
        name="stack",
        compiler_params=budget(4),
    )(*hold(own, *received))


def assemble(entries, start=None):
    count = len(entries)
    extra = 0 if start is None else 2

    def body(*refs):
        core = lax.axis_index("c")
        owners = (lax.axis_index("x"), lax.axis_index("z"))
        pieces = refs[: 2 * count]
        outs = refs[2 * count + extra : 2 * count + extra + 2]
        sems = refs[2 * count + extra + 2]

        def copies(which):
            made = []
            for i, (k, first, own, _) in enumerate(entries):
                for at, gradient in ((2 * i, which), (2 * i + 1, 1 - which)):
                    member = (owners[gradient] - k + 4) % 4
                    rows = pl.ds(pl.multiple_of(member * 1024 + first, 512), own.shape[0])
                    made.append(
                        pltpu.make_async_copy(pieces[at], outs[gradient].at[rows, :], sems.at[at])
                    )
            return made

        for which in (0, 1):

            @pl.when(core == which)
            def _():
                made = copies(which)
                for copy in made:
                    copy.start()
                for copy in made:
                    copy.wait()

    anywhere = pl.BlockSpec(memory_space=pl.ANY)
    blocks = [block for entry in entries for block in entry[2:]]
    return pl.pallas_call(
        body,
        in_specs=[vmem()] * (2 * count) + [anywhere] * extra,
        out_specs=[anywhere] * 2,
        out_shape=[shape((WIDTH, COLS), bf16)] * 2,
        scratch_shapes=[pltpu.SemaphoreType.DMA((2 * count,))],
        input_output_aliases={} if start is None else {2 * count: 0, 2 * count + 1: 1},
        name="assemble",
        compiler_params=budget(4),
    )(*hold(*blocks), *(() if start is None else start))


def swap(value, axis):
    return lax.ppermute(value, axis, [(0, 1), (1, 0)])


def ring(value, stage, steps):
    pairs = []
    for z in range(4):
        for x in range(4):
            for c in range(2):
                along_x = (c == 0) == (stage == 1)
                to = (z, (x + steps) % 4) if along_x else ((z + steps) % 4, x)
                pairs.append(((z * 4 + x) * 2 + c, (to[0] * 4 + to[1]) * 2 + c))
    return lax.ppermute(value, ("z", "x", "c"), pairs)


def down(value):
    return lax.ppermute(value, "s", [(1, 0)])


def send_all(sends, stage):
    got = [None] * 3
    for k in (1, 3, 2):
        got[k - 1] = ring(sends[k - 1], stage, k)
    return got


def all_steps(layer_inputs, norm_gain, queries, output_gradient, w_key, value_matrix, top_grad):
    x, wk, wv = layer_inputs[0], w_key[0], value_matrix[0]
    normed, keys, values, inverse, x, wk, wv = project(x, norm_gain, wk, wv)
    theirs = swap(normed, "c")
    gk, gv, keep, send, row = attend(queries[0], output_gradient[0], keys, values)
    operands = (normed, theirs, keep, swap(send, "c"))
    top, bottom = weight_far(*operands)
    top, bottom = ring(top, 1, 1), ring(bottom, 1, 3)
    a_top, a_bottom, b_top, b_bottom = weight_near(*operands)
    from_bottom, from_top = ring(a_bottom, 1, 1), ring(b_top, 1, 3)
    kept = weight_own(*operands)
    a_top, b_bottom = relay(a_top, top), relay(b_bottom, bottom)
    halves = (ring(a_top, 1, 1), from_bottom, from_top, ring(b_bottom, 1, 3))
    own, lower, upper = input_terms(gk, gv, wk, wv, x, top_grad, norm_gain, inverse, row)
    lower_got = down(lower)
    kept, *sends = sum_parts(kept, *halves)
    got = send_all(sends, 2)
    part = total(kept, got)
    block = mean(part, swap(part, "y"))
    upper_got = down(upper)
    got = send_all([block] * 3, 2)
    top, bottom = stack(block, got)
    behind_top, ahead_bottom = ring(top, 1, 1), ring(bottom, 1, 3)
    behind_bottom, ahead_top = ring(bottom, 1, 1), ring(top, 1, 3)
    blocks = (
        (0, 0, top),
        (0, 512, bottom),
        (1, 0, behind_top),
        (3, 512, ahead_bottom),
        (1, 512, behind_bottom),
        (3, 0, ahead_top),
        (2, 0, ring(behind_top, 1, 1)),
        (2, 512, ring(ahead_bottom, 1, 3)),
    )
    entries = [(k, first, block, swap(block, "c")) for k, first, block in blocks]
    part = assemble(entries[:2])
    part = assemble(entries[2:4], part)
    part = assemble(entries[4:6], part)
    value_grad, key_grad = assemble(entries[6:], part)
    input_grad = finish(own, lower_got, upper_got)
    return (key_grad[None], value_grad[None], input_grad[None])


def solution(mesh):
    wide = Mesh(mesh.devices.reshape(2, 4, 4, 2, 2), ("s", "z", "x", "y", "c"))
    dp = ("z", "x", "y", "c")
    in_specs = (
        P("s", dp, None),
        P("s", None),
        P("s", dp, None),
        P("s", dp, None),
        P("s", None, None),
        P("s", None, None),
        P(dp, None),
    )
    out_specs = (P("s", None, None), P("s", None, None), P("s", dp, None))
    return jax.shard_map(all_steps, mesh=wide, in_specs=in_specs, out_specs=out_specs, check_vma=False)
```
